32 devices in a mesh: shard: 8 (over z, y), model: 4 (over x, core).
Axes of the slice: x: 2, y: 2, z: 4, core: 2. Of those that a mesh axis runs over, the one named last changes fastest.
Arguments:
- one_gate: float32 [2048, 8192], P('shard', 'model'), may hold values from -0.1875 to 0.1875
- other_gate: float32 [2048, 8192], P('shard', 'model'), may hold values from -0.125 to 0.125
- one_up: float32 [2048, 8192], P('shard', 'model'), may hold values from -0.1875 to 0.1875
- other_up: float32 [2048, 8192], P('shard', 'model'), may hold values from -0.125 to 0.125
- mix_share: float32 [2048], P('shard'), may hold values from 0.2 to 0.8
- norm_train: float32 [2048], P(('shard', 'model')), may hold values from 0.25 to 1.75
- norm_step: float32 [2048], P(('shard', 'model')), may hold values from -0.3 to 0.3
Outputs:
- final_gate: bfloat16 [2048, 8192], P(None, 'model')
- final_up: bfloat16 [2048, 8192], P(None, 'model')
- column_gate: float32 [8192], P('model')
- column_up: float32 [8192], P('model')
- serve_norm: bfloat16 [2048], replicated
The draws below stay inside these ranges and needn't reach their ends.
All inputs are finite; a program needn't handle non-finite values. Where the reference program divides by a largest or mean magnitude, that divisor is 1e-20 or more.
Results may differ from the reference program's by a relative error of at most 0.001.
Values may be sent and summed in bfloat16 or wider, within the bound.
A program may use at most 128 MiB of HBM per device.

```python
import jax
import jax.numpy as jnp

D_MODEL = 2048
D_INNER = 8192


def spiked(entries, rng, source, target, blocks, factor):
    def block_of(position):
        return (jnp.arange(entries.shape[position]) // (entries.shape[position] // blocks)).reshape((-1,) + (1,) * (entries.ndim - 1 - position))

    first = jax.random.permutation(rng, blocks)[block_of(target)]
    far = (block_of(target) + blocks // 2) % blocks
    return jnp.where((block_of(source) == first) | (block_of(source) == far), factor * entries, entries)


def level_of(rng, extent, shards, smallest, top_value):
    gain = 1.0
    for axis_at, parts in shards:
        draws = jax.random.uniform(jax.random.fold_in(jax.random.fold_in(rng, 6), axis_at), (parts,), jnp.float32, smallest / len(shards), top_value / len(shards))
        gain = gain * jnp.repeat(jnp.exp(draws), extent[axis_at] // parts).reshape((-1,) + (1,) * (len(extent) - 1 - axis_at))
    return gain


def centred(own_key, shape, scale, reach, split=(), held_as=jnp.bfloat16):
    values = scale * jax.random.normal(own_key, shape, jnp.float32)
    if split:
        values = values * level_of(own_key, shape, split, -0.22, 0.18)
    return jnp.clip(values, -reach, reach).astype(held_as)


def bell_draw_with(own_key, shape, width, limit, shards, heavy, kind=jnp.bfloat16):
    values = width * jax.random.normal(own_key, shape, jnp.float32)
    if shards:
        values = values * level_of(own_key, shape, shards, -0.22, 0.18)
    return jnp.clip(spiked(values, jax.random.fold_in(own_key, 3), *heavy), -limit, limit).astype(kind)


def setup_inputs(seed: int = 0) -> dict:
    keys = jax.random.split(jax.random.key(seed), 8)
    one_gate = bell_draw_with(keys[0], (D_MODEL, D_INNER), D_MODEL ** -0.5, 0.1875, ((0, 8), (1, 4)), (0, 1, 8, 2.0), jnp.float32)
    other_gate = centred(keys[1], (D_MODEL, D_INNER), D_MODEL ** -0.5, 0.125, ((0, 8), (1, 4)), jnp.float32)
    one_up = bell_draw_with(keys[2], (D_MODEL, D_INNER), D_MODEL ** -0.5, 0.1875, ((0, 8), (1, 4)), (0, 1, 8, 2.0), jnp.float32)
    other_up = centred(keys[3], (D_MODEL, D_INNER), D_MODEL ** -0.5, 0.125, ((0, 8), (1, 4)), jnp.float32)
    mix_share = jnp.clip(0.2 + 0.6 * jax.random.uniform(keys[4], (D_MODEL,), jnp.float32) ** level_of(keys[4], (D_MODEL,), ((0, 8),), -0.2, 0.2), 0.2, 0.8)
    norm_train = jnp.clip(1.0 + 0.15 * jax.random.normal(keys[5], (D_MODEL,), jnp.float32), 0.25, 1.75)
    norm_step = jnp.clip(jax.random.uniform(keys[6], (D_MODEL,), jnp.float32, -0.3, 0.3) * level_of(keys[6], (D_MODEL,), ((0, 32),), -0.4, 0.0), -0.3, 0.3)
    return {"one_gate": one_gate, "other_gate": other_gate, "one_up": one_up, "other_up": other_up, "mix_share": mix_share, "norm_train": norm_train, "norm_step": norm_step}


def reference(one_gate, other_gate, one_up, other_up, mix_share, norm_train, norm_step):
    result_gate = mix_share[:, None] * one_gate + (1.0 - mix_share[:, None]) * other_gate
    result_up = mix_share[:, None] * one_up + (1.0 - mix_share[:, None]) * other_up
    column_gate = jnp.max(jnp.abs(result_gate), axis=0)
    final_gate = (result_gate / column_gate).astype(jnp.bfloat16)
    column_up = jnp.max(jnp.abs(result_up), axis=0)
    final_up = (result_up / column_up).astype(jnp.bfloat16)
    serve_norm = (norm_train + norm_step).astype(jnp.bfloat16)
    return final_gate, final_up, column_gate, column_up, serve_norm
```

```python
import functools

import jax
import jax.numpy as jnp
from jax import lax
from jax.experimental import pallas as pl
from jax.experimental.pallas import tpu as pltpu
from jax.sharding import PartitionSpec as P

MESH = pl.DeviceIdType.MESH
LANES = 128


def position_of(index, n):
    return jnp.where(index % 2 == 0, index // 2, n - 1 - index // 2)


def index_at(position, n):
    return jnp.where(position < n // 2, 2 * position, 2 * (n - 1 - position) + 1)


def kernel(
    n, k, parts,
    one_gate, other_gate, one_up, other_up, mix, norm_train, norm_step,
    final_gate, final_up, column_gate, column_up, serve_norm,
    held_one, held_other, share, maxima, gains, gain_rows,
    load_sem, max_send, max_recv, norm_send, norm_recv, ring_send, ring_recv,
):
    rows, cols = one_gate.shape
    piece = norm_train.shape[1]
    part = cols // parts
    me, col = lax.axis_index("shard"), lax.axis_index("model")
    at = position_of(me, n)

    ones, others = (one_gate, one_up), (other_gate, other_up)
    finals, columns = (final_gate, final_up), (column_gate, column_up)

    loads = {}
    for w in range(2):
        for c in range(parts):
            span = pl.ds(c * part, part)
            pair = (
                pltpu.make_async_copy(ones[w].at[:, span], held_one.at[w, :, span], load_sem.at[w, c, 0]),
                pltpu.make_async_copy(others[w].at[:, span], held_other.at[w, :, span], load_sem.at[w, c, 1]),
            )
            for copy in pair:
                copy.start()
            loads[w, c] = pair

    barrier = pltpu.get_barrier_semaphore()
    for d in range(1, n):
        pl.semaphore_signal(barrier, inc=1, device_id=((me + d) % n, col), device_id_type=MESH)
    for d in range(1, k):
        pl.semaphore_signal(barrier, inc=1, device_id=(me, (col + d) % k), device_id_type=MESH)

    share[...] = jnp.broadcast_to(mix[...], (LANES, rows)).T

    maxima[1, parts - 1, 0, :, part:part + piece] = norm_train[...] + norm_step[...]

    def mixed(w, c):
        for copy in loads[w, c]:
            copy.wait()
        span = pl.ds(c * part, part)

        def step(g, top):
            lines = pl.ds(pl.multiple_of(g * 8, 8), 8)
            m = share[lines, 0:1]
            result = m * held_one[w, lines, span] + (1.0 - m) * held_other[w, lines, span]
            held_one[w, lines, span] = result
            return jnp.maximum(top, jnp.abs(result))

        top = lax.fori_loop(0, rows // 8, step, jnp.zeros((8, part), jnp.float32), unroll=4)
        maxima[w, c, 0, :, 0:part] = jnp.max(top, axis=0, keepdims=True)

    def tell(w, c):
        width = part + LANES if (w, c) == (1, parts - 1) else part
        copies = []
        for d in range(1, n):
            copy = pltpu.make_async_remote_copy(
                src_ref=maxima.at[w, c, 0, :, pl.ds(0, width)], dst_ref=maxima.at[w, c, d, :, pl.ds(0, width)],
                send_sem=max_send.at[w, c, d], recv_sem=max_recv.at[w, c, d],
                device_id=((me + d) % n, col), device_id_type=MESH,
            )
            copy.start()
            copies.append(copy)
        return copies

    def ring(way, hop, w, c):
        origin = index_at((at + (n - hop if way == 0 else hop)) % n, n)
        lines, span = pl.ds(pl.multiple_of(origin * rows, rows), rows), pl.ds(c * part, part)
        to = index_at((at + (1 if way == 0 else n - 1)) % n, n)
        return pltpu.make_async_remote_copy(
            src_ref=finals[w].at[lines, span], dst_ref=finals[w].at[lines, span],
            send_sem=ring_send.at[way, hop, w, c], recv_sem=ring_recv.at[way, hop, w, c],
            device_id=(to, col), device_id_type=MESH,
        )

    def scaled(w, c, inverse):
        span = pl.ds(c * part, part)

        def step(g, _):
            start = pl.multiple_of(g * 16, 16)
            to = pl.multiple_of(me * rows + g * 16, 16)
            finals[w][pl.ds(to, 16), span] = (held_one[w, pl.ds(start, 16), span] * inverse).astype(jnp.bfloat16)
            return 0

        lax.fori_loop(0, rows // 16, step, 0, unroll=2)

    units = [(w, c) for w in range(2) for c in range(parts)]
    told = {}
    for w, c in units:
        mixed(w, c)
        if (w, c) == units[0]:
            pl.semaphore_wait(barrier, n - 1 + k - 1)
        told[w, c] = tell(w, c)

    sent, norms = {}, []
    for w, c in units:
        for copy in told[w, c]:
            copy.wait_recv()
        column = jnp.max(maxima[w, c, :, :, 0:part], axis=0)
        columns[w][:, pl.ds(c * part, part)] = column
        scaled(w, c, 1.0 / column)
        for way in range(2):
            sent[way, 0, w, c] = ring(way, 0, w, c)
            sent[way, 0, w, c].start()

    for d in range(n):
        gains[0, pl.ds((me + (n - d)) % n, 1), :] = maxima[1, parts - 1, d, :, part:part + LANES]
    for d in range(1, k):
        copy = pltpu.make_async_remote_copy(
            src_ref=gains.at[0], dst_ref=gains.at[d],
            send_sem=norm_send.at[d], recv_sem=norm_recv.at[d],
            device_id=(me, (col + d) % k), device_id_type=MESH,
        )
        copy.start()
        norms.append(copy)
    for copy in norms:
        copy.wait_recv()
    gain = jnp.concatenate([gains[(col + (k - j)) % k][:, 0:piece] for j in range(k)], axis=1)
    if serve_norm.shape[1] == gain.shape[1]:
        serve_norm[...] = gain.astype(jnp.bfloat16)
    else:
        each = k * piece // LANES
        for i in range(n * each):
            at_lane = i % each * LANES
            gain_rows[i:i + 1, :] = gain[i // each:i // each + 1, at_lane:at_lane + LANES]
        serve_norm[...] = gain_rows[...].astype(jnp.bfloat16)

    for hop in range(1, n // 2 + 1):
        for w in range(2):
            for c in range(parts):
                for way in range(2):
                    if (way, hop - 1, w, c) not in sent:
                        continue
                    sent[way, hop - 1, w, c].wait_recv()
                    if hop < n // 2 - 1 or (hop == n // 2 - 1 and way == w):
                        sent[way, hop, w, c] = ring(way, hop, w, c)
                        sent[way, hop, w, c].start()

    for copy in sent.values():
        copy.wait_send()
    for copy in sum(told.values(), norms):
        copy.wait_send()


def near_kernel(
    n, k, units, early,
    one_gate, other_gate, one_up, other_up, mix, norm_train, norm_step,
    final_gate, final_up, column_gate, column_up, serve_norm,
    held_one, held_other, mix_held, train_held, step_held, share, raw, maxima, gains, gain_rows,
    load_sem, small_sem, raw_send, raw_recv, max_send, max_recv, norm_send, norm_recv, ring_send, ring_recv,
):
    rows, cols = one_gate.shape
    piece = norm_train.shape[1]
    me, col = lax.axis_index("shard"), lax.axis_index("model")
    at = position_of(me, n)

    ones, others = (one_gate, one_up), (other_gate, other_up)
    finals, columns = (final_gate, final_up), (column_gate, column_up)

    smalls = (
        pltpu.make_async_copy(mix, mix_held, small_sem.at[0]),
        pltpu.make_async_copy(norm_train, train_held, small_sem.at[1]),
        pltpu.make_async_copy(norm_step, step_held, small_sem.at[2]),
    )
    smalls[0].start()

    loads = {}

    def load(u):
        w, first, width = units[u]
        span = pl.ds(first, width)
        loads[u] = (
            pltpu.make_async_copy(ones[w].at[:, span], held_one.at[w, :, span], load_sem.at[u, 0]),
            pltpu.make_async_copy(others[w].at[:, span], held_other.at[w, :, span], load_sem.at[u, 1]),
        )
        for copy in loads[u]:
            copy.start()

    load(0)
    barrier = pltpu.get_barrier_semaphore()
    for d in range(n - 1, 0, -1):
        pl.semaphore_signal(barrier, inc=1, device_id=((me + d) % n, col), device_id_type=MESH)
    for d in range(1, k):
        pl.semaphore_signal(barrier, inc=1, device_id=(me, (col + d) % k), device_id_type=MESH)
    load(early)
    for u in range(1, len(units)):
        if u != early:
            load(u)
    for copy in smalls[1:]:
        copy.start()

    smalls[0].wait()
    share[...] = jnp.broadcast_to(mix_held[...], (LANES, rows)).T

    def mixed(u):
        for copy in loads[u]:
            copy.wait()
        w, first, width = units[u]
        span = pl.ds(first, width)

        def step(g, top):
            lines = pl.ds(pl.multiple_of(g * 8, 8), 8)
            m = share[lines, :]
            both = jnp.concatenate([m] * (width // LANES), axis=1)
            rest = jnp.concatenate([1.0 - m] * (width // LANES), axis=1)
            result = both * held_one[w, lines, span] + rest * held_other[w, lines, span]
            held_one[w, lines, span] = result
            return jnp.maximum(top, jnp.abs(result))

        top = lax.fori_loop(0, rows // 8, step, jnp.zeros((8, width), jnp.float32), unroll=4)
        maxima[w, 0, :, span] = jnp.max(top, axis=0, keepdims=True)

    def tell(u):
        w, first, width = units[u]
        span = pl.ds(first, width + LANES if u == early else width)
        copies = []
        for d in range(1, n):
            copy = pltpu.make_async_remote_copy(
                src_ref=maxima.at[w, 0, :, span], dst_ref=maxima.at[w, d, :, span],
                send_sem=max_send.at[u, d], recv_sem=max_recv.at[u, d],
                device_id=((me + d) % n, col), device_id_type=MESH,
            )
            copy.start()
            copies.append(copy)
        return copies

    def toward(way):
        return index_at((at + (1 if way == 0 else n - 1)) % n, n)

    def origin_of(way, hop):
        return index_at((at + (n - hop if way == 0 else hop)) % n, n)

    def ring(way, hop, u):
        w, first, width = units[u]
        lines = pl.ds(pl.multiple_of(origin_of(way, hop) * rows, rows), rows)
        span = pl.ds(first, width)
        return pltpu.make_async_remote_copy(
            src_ref=finals[w].at[lines, span], dst_ref=finals[w].at[lines, span],
            send_sem=ring_send.at[way, hop, u], recv_sem=ring_recv.at[way, hop, u],
            device_id=(toward(way), col), device_id_type=MESH,
        )

    def ahead(way):
        w, first, width = units[early]
        return pltpu.make_async_remote_copy(
            src_ref=held_one.at[w, :, pl.ds(first, width)], dst_ref=raw.at[way],
            send_sem=raw_send.at[way], recv_sem=raw_recv.at[way],
            device_id=(toward(way), col), device_id_type=MESH,
        )

    def scaled(u, origin, inverse, read):
        w, first, width = units[u]

        def step(g, _):
            start = pl.multiple_of(g * 16, 16)
            to = pl.multiple_of(origin * rows + g * 16, 16)
            finals[w][pl.ds(to, 16), pl.ds(first, width)] = (read(pl.ds(start, 16)) * inverse).astype(jnp.bfloat16)
            return 0

        lax.fori_loop(0, rows // 16, step, 0, unroll=2)

    def scale_of(u):
        for copy in told[u]:
            copy.wait_recv()
        w, first, width = units[u]
        span = pl.ds(first, width)
        column = jnp.max(maxima[w, :, :, span], axis=0)
        columns[w][:, span] = column
        return 1.0 / column

    told, sent, norms = {}, {}, []
    mixed(0)
    pl.semaphore_wait(barrier, n - 1 + k - 1)
    told[0] = tell(0)
    mixed(early)
    aheads = [ahead(way) for way in range(2)]
    for copy in aheads:
        copy.start()
    for copy in smalls[1:]:
        copy.wait()
    maxima[units[early][0], 0, :, cols:cols + piece] = train_held[...] + step_held[...]
    for u in range(1, len(units)):
        if u != early:
            mixed(u)
        told[u] = tell(u)

    order = [u for u in range(len(units)) if u != early]
    for u in order:
        w, first, width = units[u]
        inverse = scale_of(u)
        scaled(u, me, inverse, lambda lines: held_one[w, lines, pl.ds(first, width)])
        for way in range(2):
            sent[way, 0, u] = ring(way, 0, u)
            sent[way, 0, u].start()

    w, first, width = units[early]
    inverse = scale_of(early)
    for way in range(2):
        aheads[way].wait_recv()
        scaled(early, origin_of(way, 1), inverse, lambda lines: raw[way, lines, :])
        sent[way, 1, early] = ring(way, 1, early)
        sent[way, 1, early].start()
    scaled(early, me, inverse, lambda lines: held_one[w, lines, pl.ds(first, width)])

    for d in range(n):
        gains[0, pl.ds((me + (n - d)) % n, 1), :] = maxima[units[early][0], d, :, cols:cols + LANES]
    for d in range(1, k):
        copy = pltpu.make_async_remote_copy(
            src_ref=gains.at[0], dst_ref=gains.at[d],
            send_sem=norm_send.at[d], recv_sem=norm_recv.at[d],
            device_id=(me, (col + d) % k), device_id_type=MESH,
        )
        copy.start()
        norms.append(copy)
    for copy in norms:
        copy.wait_recv()
    gain = jnp.concatenate([gains[(col + (k - j)) % k][:, 0:piece] for j in range(k)], axis=1)
    if serve_norm.shape[1] == gain.shape[1]:
        serve_norm[...] = gain.astype(jnp.bfloat16)
    else:
        each = k * piece // LANES
        for i in range(n * each):
            at_lane = i % each * LANES
            gain_rows[i:i + 1, :] = gain[i // each:i // each + 1, at_lane:at_lane + LANES]
        serve_norm[...] = gain_rows[...].astype(jnp.bfloat16)

    for hop in range(1, n // 2 + 1):
        for u in order + [early]:
            for way in range(2):
                if (way, hop - 1, u) not in sent:
                    continue
                sent[way, hop - 1, u].wait_recv()
                if hop < n // 2 - 1 or (hop == n // 2 - 1 and way == units[u][0]):
                    sent[way, hop, u] = ring(way, hop, u)
                    sent[way, hop, u].start()

    for copy in list(sent.values()) + aheads:
        copy.wait_send()
    for copy in sum(told.values(), norms):
        copy.wait_send()


def writer(*refs):
    (sem,), count = refs[-1:], (len(refs) - 1) // 2
    copies = []
    for source, target in zip(refs[:count], refs[count:-1]):
        pieces = 4 if source.shape[0] > LANES else 1
        lines = source.shape[0] // pieces
        for p in range(pieces):
            span = pl.ds(p * lines, lines)
            copies.append(pltpu.make_async_copy(source.at[span], target.at[span], sem.at[len(copies)]))
    for copy in copies:
        copy.start()
    for copy in copies:
        copy.wait()


def solution(mesh):
    n, k = mesh.shape["shard"], mesh.shape["model"]

    def local(one_gate, other_gate, one_up, other_up, mix_share, norm_train, norm_step):
        rows, cols = one_gate.shape
        piece = norm_train.shape[0]
        parts = 2 if n <= 8 else 1
        near = n <= 8
        shaped = pltpu.VMEM if near else jax.ShapeDtypeStruct
        norm_shape = (n * k * piece // LANES, LANES) if k * piece % LANES == 0 else (n, k * piece)
        shapes = [
            ((n * rows, cols), jnp.bfloat16), ((n * rows, cols), jnp.bfloat16),
            ((1, cols), jnp.float32), ((1, cols), jnp.float32), (norm_shape, jnp.bfloat16),
        ]
        hbm, vmem = pl.BlockSpec(memory_space=pltpu.HBM), pl.BlockSpec(memory_space=pltpu.VMEM)
        e = cols // 8
        units = ((0, 0, 2 * e), (0, 2 * e, 2 * e), (0, 4 * e, 4 * e), (1, 0, 4 * e), (1, 4 * e, 3 * e), (1, 7 * e, e))
        early = len(units) - 1
        common = [
            pltpu.VMEM((2, rows, cols), jnp.float32),
            pltpu.VMEM((2, rows, cols), jnp.float32),
        ]
        gain_shapes = [
            pltpu.VMEM((k, n, LANES), jnp.float32),
            pltpu.VMEM((max(n * k * piece // LANES, 8), LANES), jnp.float32),
        ]
        sems = pltpu.SemaphoreType.DMA
        if near:
            body = functools.partial(near_kernel, n, k, units, early)
            small_spec = hbm
            scratch = common + [
                pltpu.VMEM((1, rows), jnp.float32), pltpu.VMEM((1, piece), jnp.float32), pltpu.VMEM((1, piece), jnp.float32),
                pltpu.VMEM((rows, LANES), jnp.float32),
                pltpu.VMEM((2, rows, e), jnp.float32),
                pltpu.VMEM((2, n, 1, cols + LANES), jnp.float32),
            ] + gain_shapes + [
                sems((len(units), 2)), sems((3,)), sems((2,)), sems((2,)),
                sems((len(units), n)), sems((len(units), n)), sems((k,)), sems((k,)),
                sems((2, n // 2, len(units))), sems((2, n // 2, len(units))),
            ]
        else:
            body = functools.partial(kernel, n, k, parts)
            small_spec = vmem
            scratch = common + [
                pltpu.VMEM((rows, LANES), jnp.float32),
                pltpu.VMEM((2, parts, n, 1, cols // parts + LANES), jnp.float32),
            ] + gain_shapes + [
                sems((2, parts, 2)), sems((2, parts, n)), sems((2, parts, n)), sems((k,)), sems((k,)),
                sems((2, n // 2, 2, parts)), sems((2, n // 2, 2, parts)),
            ]
        results = pl.pallas_call(
            body,
            out_shape=[shaped(*shape) for shape in shapes],
            in_specs=[hbm] * 4 + [small_spec] * 3,
            out_specs=[vmem] * 5,
            scratch_shapes=scratch,
            compiler_params=pltpu.CompilerParams(
                collective_id=0, has_side_effects=True, vmem_limit_bytes=46 * 2**20
            ),
        )(
            one_gate, other_gate, one_up, other_up,
            mix_share.reshape(1, rows), norm_train.reshape(1, piece), norm_step.reshape(1, piece),
        )
        if near:
            results = pl.pallas_call(
                writer,
                out_shape=[jax.ShapeDtypeStruct(*shape) for shape in shapes],
                in_specs=[vmem] * 5,
                out_specs=[hbm] * 5,
                scratch_shapes=[pltpu.SemaphoreType.DMA((11,))],
                compiler_params=pltpu.CompilerParams(vmem_limit_bytes=2**20),
            )(*results)
        final_gate, final_up, column_gate, column_up, serve_norm = results
        return (
            final_gate, final_up, column_gate.reshape(cols), column_up.reshape(cols),
            serve_norm.reshape(n * k * piece),
        )

    return jax.shard_map(
        local,
        mesh=mesh,
        in_specs=(
            P("shard", "model"), P("shard", "model"), P("shard", "model"), P("shard", "model"),
            P("shard"), P(("shard", "model")), P(("shard", "model")),
        ),
        out_specs=(P(None, "model"), P(None, "model"), P("model"), P("model"), P()),
        check_vma=False,
    )
```

```python
import functools

import jax
import jax.numpy as jnp
from jax import lax
from jax.experimental import pallas as pl
from jax.experimental.pallas import tpu as pltpu
from jax.sharding import PartitionSpec as P

MESH = pl.DeviceIdType.MESH
LANES = 128


def position_of(index, n):
    return jnp.where(index % 2 == 0, index // 2, n - 1 - index // 2)


def index_at(position, n):
    return jnp.where(position < n // 2, 2 * position, 2 * (n - 1 - position) + 1)


def kernel(
    n, k, parts,
    one_gate, other_gate, one_up, other_up, mix, norm_train, norm_step,
    final_gate, final_up, column_gate, column_up, serve_norm,
    held_one, held_other, share, maxima, gains, gain_rows,
    load_sem, max_send, max_recv, norm_send, norm_recv, ring_send, ring_recv,
):
    rows, cols = one_gate.shape
    piece = norm_train.shape[1]
    part = cols // parts
    me, col = lax.axis_index("shard"), lax.axis_index("model")
    at = position_of(me, n)

    ones, others = (one_gate, one_up), (other_gate, other_up)
    finals, columns = (final_gate, final_up), (column_gate, column_up)

    loads = {}
    for w in range(2):
        for c in range(parts):
            span = pl.ds(c * part, part)
            pair = (
                pltpu.make_async_copy(ones[w].at[:, span], held_one.at[w, :, span], load_sem.at[w, c, 0]),
                pltpu.make_async_copy(others[w].at[:, span], held_other.at[w, :, span], load_sem.at[w, c, 1]),
            )
            for copy in pair:
                copy.start()
            loads[w, c] = pair

    barrier = pltpu.get_barrier_semaphore()
    for d in range(1, n):
        pl.semaphore_signal(barrier, inc=1, device_id=((me + d) % n, col), device_id_type=MESH)
    for d in range(1, k):
        pl.semaphore_signal(barrier, inc=1, device_id=(me, (col + d) % k), device_id_type=MESH)

    share[...] = jnp.broadcast_to(mix[...], (LANES, rows)).T

    maxima[1, parts - 1, 0, :, part:part + piece] = norm_train[...] + norm_step[...]

    def mixed(w, c):
        for copy in loads[w, c]:
            copy.wait()
        span = pl.ds(c * part, part)

        def step(g, top):
            lines = pl.ds(pl.multiple_of(g * 8, 8), 8)
            m = share[lines, 0:1]
            result = m * held_one[w, lines, span] + (1.0 - m) * held_other[w, lines, span]
            held_one[w, lines, span] = result
            return jnp.maximum(top, jnp.abs(result))

        top = lax.fori_loop(0, rows // 8, step, jnp.zeros((8, part), jnp.float32), unroll=4)
        maxima[w, c, 0, :, 0:part] = jnp.max(top, axis=0, keepdims=True)

    def tell(w, c):
        width = part + LANES if (w, c) == (1, parts - 1) else part
        copies = []
        for d in range(1, n):
            copy = pltpu.make_async_remote_copy(
                src_ref=maxima.at[w, c, 0, :, pl.ds(0, width)], dst_ref=maxima.at[w, c, d, :, pl.ds(0, width)],
                send_sem=max_send.at[w, c, d], recv_sem=max_recv.at[w, c, d],
                device_id=((me + d) % n, col), device_id_type=MESH,
            )
            copy.start()
            copies.append(copy)
        return copies

    def ring(way, hop, w, c):
        origin = index_at((at + (n - hop if way == 0 else hop)) % n, n)
        lines, span = pl.ds(pl.multiple_of(origin * rows, rows), rows), pl.ds(c * part, part)
        to = index_at((at + (1 if way == 0 else n - 1)) % n, n)
        return pltpu.make_async_remote_copy(
            src_ref=finals[w].at[lines, span], dst_ref=finals[w].at[lines, span],
            send_sem=ring_send.at[way, hop, w, c], recv_sem=ring_recv.at[way, hop, w, c],
            device_id=(to, col), device_id_type=MESH,
        )

    def scaled(w, c, inverse):
        span = pl.ds(c * part, part)

        def step(g, _):
            start = pl.multiple_of(g * 16, 16)
            to = pl.multiple_of(me * rows + g * 16, 16)
            finals[w][pl.ds(to, 16), span] = (held_one[w, pl.ds(start, 16), span] * inverse).astype(jnp.bfloat16)
            return 0

        lax.fori_loop(0, rows // 16, step, 0, unroll=2)

    units = [(w, c) for w in range(2) for c in range(parts)]
    told = {}
    for w, c in units:
        mixed(w, c)
        if (w, c) == units[0]:
            pl.semaphore_wait(barrier, n - 1 + k - 1)
        told[w, c] = tell(w, c)

    sent, norms = {}, []
    for w, c in units:
        for copy in told[w, c]:
            copy.wait_recv()
        column = jnp.max(maxima[w, c, :, :, 0:part], axis=0)
        columns[w][:, pl.ds(c * part, part)] = column
        scaled(w, c, 1.0 / column)
        for way in range(2):
            sent[way, 0, w, c] = ring(way, 0, w, c)
            sent[way, 0, w, c].start()

    for d in range(n):
        gains[0, pl.ds((me + (n - d)) % n, 1), :] = maxima[1, parts - 1, d, :, part:part + LANES]
    for d in range(1, k):
        copy = pltpu.make_async_remote_copy(
            src_ref=gains.at[0], dst_ref=gains.at[d],
            send_sem=norm_send.at[d], recv_sem=norm_recv.at[d],
            device_id=(me, (col + d) % k), device_id_type=MESH,
        )
        copy.start()
        norms.append(copy)
    for copy in norms:
        copy.wait_recv()
    gain = jnp.concatenate([gains[(col + (k - j)) % k][:, 0:piece] for j in range(k)], axis=1)
    if serve_norm.shape[1] == gain.shape[1]:
        serve_norm[...] = gain.astype(jnp.bfloat16)
    else:
        each = k * piece // LANES
        for i in range(n * each):
            at_lane = i % each * LANES
            gain_rows[i:i + 1, :] = gain[i // each:i // each + 1, at_lane:at_lane + LANES]
        serve_norm[...] = gain_rows[...].astype(jnp.bfloat16)

    for hop in range(1, n // 2 + 1):
        for w in range(2):
            for c in range(parts):
                for way in range(2):
                    if (way, hop - 1, w, c) not in sent:
                        continue
                    sent[way, hop - 1, w, c].wait_recv()
                    if hop < n // 2 - 1 or (hop == n // 2 - 1 and way == w):
                        sent[way, hop, w, c] = ring(way, hop, w, c)
                        sent[way, hop, w, c].start()

    for copy in sent.values():
        copy.wait_send()
    for copy in sum(told.values(), norms):
        copy.wait_send()


def near_kernel(
    n, k, units, direct, early,
    one_gate, other_gate, one_up, other_up, mix, norm_train, norm_step,
    final_gate, final_up, column_gate, column_up, serve_norm,
    held_one, held_other, result, mix_held, train_held, step_held, share, raw, mine, heard, partial, whole, gains, gain_rows,
    load_sem, small_sem, raw_send, raw_recv, max_send, max_recv, part_send, part_recv, whole_send, whole_recv,
    norm_send, norm_recv, ring_send, ring_recv,
):
    rows, cols = one_gate.shape
    piece = norm_train.shape[1]
    block = mine.shape[2]
    me, col = lax.axis_index("shard"), lax.axis_index("model")
    at = position_of(me, n)

    ones, others = (one_gate, one_up), (other_gate, other_up)
    finals, columns = (final_gate, final_up), (column_gate, column_up)

    def peer(d):
        return ((me + d) % n, col)

    smalls = (
        pltpu.make_async_copy(mix, mix_held, small_sem.at[0]),
        pltpu.make_async_copy(norm_train, train_held, small_sem.at[1]),
        pltpu.make_async_copy(norm_step, step_held, small_sem.at[2]),
    )
    loads = {}

    def load(u):
        w, first, width = units[u]
        span = pl.ds(first, width)
        loads[u] = (
            pltpu.make_async_copy(ones[w].at[:, span], held_one.at[w, :, span], load_sem.at[u, 0]),
            pltpu.make_async_copy(others[w].at[:, span], held_other.at[w, :, span], load_sem.at[u, 1]),
        )
        for copy in loads[u]:
            copy.start()

    smalls[0].start()
    load(0)
    barrier = pltpu.get_barrier_semaphore()
    for d in range(1, n):
        pl.semaphore_signal(barrier, inc=1, device_id=peer(d), device_id_type=MESH)
    for d in range(1, k):
        pl.semaphore_signal(barrier, inc=1, device_id=(me, (col + d) % k), device_id_type=MESH)
    load(early)
    for u in range(1, early):
        load(u)
    for copy in smalls[1:]:
        copy.start()

    smalls[0].wait()
    share[...] = jnp.broadcast_to(mix_held[...], (LANES, rows)).T

    def mixed(u):
        for copy in loads[u]:
            copy.wait()
        w, first, width = units[u]
        span = pl.ds(first, width)

        def step(g, top):
            lines = pl.ds(pl.multiple_of(g * 8, 8), 8)
            m = share[lines, :]
            both = jnp.concatenate([m] * (width // LANES), axis=1)
            rest = jnp.concatenate([1.0 - m] * (width // LANES), axis=1)
            value = both * held_one[w, lines, span] + rest * held_other[w, lines, span]
            result[w, lines, span] = value
            return jnp.maximum(top, jnp.abs(value))

        top = lax.fori_loop(0, rows // 8, step, jnp.zeros((8, width), jnp.float32), unroll=4)
        top = jnp.max(top, axis=0, keepdims=True)
        done = 0
        while done < width:
            b, lane = (w * cols + first + done) // block, (first + done) % block
            take = min(block - lane, width - done)
            mine[b, :, lane:lane + take] = top[:, done:done + take]
            done += take

    def tell(u):
        copies = []
        for d in range(1, n):
            copy = pltpu.make_async_remote_copy(
                src_ref=mine.at[u], dst_ref=heard.at[u, d],
                send_sem=max_send.at[u, d], recv_sem=max_recv.at[u, d], device_id=peer(d), device_id_type=MESH,
            )
            copy.start()
            copies.append(copy)
        return copies

    def toward(way):
        return index_at((at + (1 if way == 0 else n - 1)) % n, n)

    def origin_of(way, hop):
        return index_at((at + (n - hop if way == 0 else hop)) % n, n)

    def ring(way, hop, u):
        w, first, width = units[u]
        lines = pl.ds(pl.multiple_of(origin_of(way, hop) * rows, rows), rows)
        span = pl.ds(first, width)
        return pltpu.make_async_remote_copy(
            src_ref=finals[w].at[lines, span], dst_ref=finals[w].at[lines, span],
            send_sem=ring_send.at[way, hop, u], recv_sem=ring_recv.at[way, hop, u],
            device_id=(toward(way), col), device_id_type=MESH,
        )

    def ahead(way):
        w, first, width = units[early]
        return pltpu.make_async_remote_copy(
            src_ref=result.at[w, :, pl.ds(first, width)], dst_ref=raw.at[way],
            send_sem=raw_send.at[way], recv_sem=raw_recv.at[way],
            device_id=(toward(way), col), device_id_type=MESH,
        )

    def scaled(u, origin, inverse, read):
        w, first, width = units[u]

        def step(g, _):
            start = pl.multiple_of(g * 16, 16)
            to = pl.multiple_of(origin * rows + g * 16, 16)
            finals[w][pl.ds(to, 16), pl.ds(first, width)] = (read(pl.ds(start, 16)) * inverse).astype(jnp.bfloat16)
            return 0

        lax.fori_loop(0, rows // 16, step, 0, unroll=2)

    def held(u):
        w, first, width = units[u]
        return lambda lines: result[w, lines, pl.ds(first, width)]

    sent, told = {}, {}

    def begin(u, inverse):
        scaled(u, me, inverse, held(u))
        for way in range(2):
            sent[way, 0, u] = ring(way, 0, u)
            sent[way, 0, u].start()

    def heard_of(u):
        for copy in told[u]:
            copy.wait_recv()
        top = mine[u]
        for d in range(1, n):
            top = jnp.maximum(top, heard[u, d])
        return 1.0 / top

    mixed(0)
    pl.semaphore_wait(barrier, n - 1 + k - 1)
    told[0] = tell(0)
    mixed(early)
    aheads = [ahead(way) for way in range(2)]
    for copy in aheads:
        copy.start()
    for u in range(1, direct):
        mixed(u)
        told[u] = tell(u)
    for u in range(direct, early):
        mixed(u)

    parts = []
    for d in range(1, n):
        copy = pltpu.make_async_remote_copy(
            src_ref=mine.at[(me + d) % n], dst_ref=partial.at[d],
            send_sem=part_send.at[d], recv_sem=part_recv.at[d], device_id=peer(d), device_id_type=MESH,
        )
        copy.start()
        parts.append(copy)

    for copy in smalls[1:]:
        copy.wait()
    begin(0, heard_of(0))

    for copy in parts:
        copy.wait_recv()
    top = mine[me]
    for d in range(1, n):
        top = jnp.maximum(top, partial[d])
    whole[me, :, 0:block] = top
    whole[me, :, block:block + piece] = train_held[...] + step_held[...]
    wholes = []
    for d in range(1, n):
        copy = pltpu.make_async_remote_copy(
            src_ref=whole.at[me], dst_ref=whole.at[me],
            send_sem=whole_send.at[d], recv_sem=whole_recv.at[d], device_id=peer(d), device_id_type=MESH,
        )
        copy.start()
        wholes.append(copy)

    for u in range(1, direct):
        begin(u, heard_of(u))

    for d in range(1, n):
        pltpu.make_async_remote_copy(
            src_ref=whole.at[me], dst_ref=whole.at[(me + (n - d)) % n],
            send_sem=whole_send.at[d], recv_sem=whole_recv.at[d], device_id=peer(d), device_id_type=MESH,
        ).wait_recv()
    for b in range(n):
        w, first = b * block // cols, b * block % cols
        columns[w][:, first:first + block] = whole[b, :, 0:block]

    for u in range(direct, early):
        w, first, width = units[u]
        begin(u, 1.0 / columns[w][:, first:first + width])

    w, first, width = units[early]
    inverse = 1.0 / columns[w][:, first:first + width]
    for way in range(2):
        aheads[way].wait_recv()
        scaled(early, origin_of(way, 1), inverse, lambda lines: raw[way, lines, :])
        sent[way, 1, early] = ring(way, 1, early)
        sent[way, 1, early].start()
    scaled(early, me, inverse, held(early))

    norms = []
    for d in range(n):
        gains[0, d:d + 1, :] = whole[d, :, block:block + LANES]
    for d in range(1, k):
        copy = pltpu.make_async_remote_copy(
            src_ref=gains.at[0], dst_ref=gains.at[d],
            send_sem=norm_send.at[d], recv_sem=norm_recv.at[d],
            device_id=(me, (col + d) % k), device_id_type=MESH,
        )
        copy.start()
        norms.append(copy)
    for copy in norms:
        copy.wait_recv()
    gain = jnp.concatenate([gains[(col + (k - j)) % k][:, 0:piece] for j in range(k)], axis=1)
    if serve_norm.shape[1] == gain.shape[1]:
        serve_norm[...] = gain.astype(jnp.bfloat16)
    else:
        each = k * piece // LANES
        for i in range(n * each):
            at_lane = i % each * LANES
            gain_rows[i:i + 1, :] = gain[i // each:i // each + 1, at_lane:at_lane + LANES]
        serve_norm[...] = gain_rows[...].astype(jnp.bfloat16)

    for hop in range(1, n // 2 + 1):
        for u in range(len(units)):
            for way in range(2):
                if (way, hop - 1, u) not in sent:
                    continue
                sent[way, hop - 1, u].wait_recv()
                if hop < n // 2 - 1 or (hop == n // 2 - 1 and way == units[u][0]):
                    sent[way, hop, u] = ring(way, hop, u)
                    sent[way, hop, u].start()

    for copy in list(sent.values()) + aheads:
        copy.wait_send()
    for copy in sum(told.values(), norms + parts + wholes):
        copy.wait_send()


def writer(*refs):
    (sem,), count = refs[-1:], (len(refs) - 1) // 2
    copies = []
    for source, target in zip(refs[:count], refs[count:-1]):
        pieces = 4 if source.shape[0] > LANES else 1
        lines = source.shape[0] // pieces
        for p in range(pieces):
            span = pl.ds(p * lines, lines)
            copies.append(pltpu.make_async_copy(source.at[span], target.at[span], sem.at[len(copies)]))
    for copy in copies:
        copy.start()
    for copy in copies:
        copy.wait()


def solution(mesh):
    n, k = mesh.shape["shard"], mesh.shape["model"]

    def local(one_gate, other_gate, one_up, other_up, mix_share, norm_train, norm_step):
        rows, cols = one_gate.shape
        piece = norm_train.shape[0]
        parts = 2 if n <= 8 else 1
        near = n <= 8
        shaped = pltpu.VMEM if near else jax.ShapeDtypeStruct
        norm_shape = (n * k * piece // LANES, LANES) if k * piece % LANES == 0 else (n, k * piece)
        shapes = [
            ((n * rows, cols), jnp.bfloat16), ((n * rows, cols), jnp.bfloat16),
            ((1, cols), jnp.float32), ((1, cols), jnp.float32), (norm_shape, jnp.bfloat16),
        ]
        hbm, vmem = pl.BlockSpec(memory_space=pltpu.HBM), pl.BlockSpec(memory_space=pltpu.VMEM)
        block = 2 * cols // n
        e = cols // 16
        units = (
            (0, 0, block), (0, block, block), (0, 2 * block, cols - 2 * block),
            (1, 0, 8 * e), (1, 8 * e, 7 * e), (1, 15 * e, e),
        )
        direct, early = 2, len(units) - 1
        gain_shapes = [
            pltpu.VMEM((k, n, LANES), jnp.float32),
            pltpu.VMEM((max(n * k * piece // LANES, 8), LANES), jnp.float32),
        ]
        sems = pltpu.SemaphoreType.DMA
        if near:
            body = functools.partial(near_kernel, n, k, units, direct, early)
            small_spec = hbm
            scratch = [pltpu.VMEM((2, rows, cols), jnp.float32)] * 3 + [
                pltpu.VMEM((1, rows), jnp.float32), pltpu.VMEM((1, piece), jnp.float32), pltpu.VMEM((1, piece), jnp.float32),
                pltpu.VMEM((rows, LANES), jnp.float32),
                pltpu.VMEM((2, rows, e), jnp.float32),
                pltpu.VMEM((n, 1, block), jnp.float32),
                pltpu.VMEM((direct, n, 1, block), jnp.float32),
                pltpu.VMEM((n, 1, block), jnp.float32),
                pltpu.VMEM((n, 1, block + LANES), jnp.float32),
            ] + gain_shapes + [
                sems((len(units), 2)), sems((3,)), sems((2,)), sems((2,)),
                sems((direct, n)), sems((direct, n)), sems((n,)), sems((n,)), sems((n,)), sems((n,)),
                sems((k,)), sems((k,)),
                sems((2, n // 2, len(units))), sems((2, n // 2, len(units))),
            ]
        else:
            body = functools.partial(kernel, n, k, parts)
            small_spec = vmem
            scratch = [pltpu.VMEM((2, rows, cols), jnp.float32)] * 2 + [
                pltpu.VMEM((rows, LANES), jnp.float32),
                pltpu.VMEM((2, parts, n, 1, cols // parts + LANES), jnp.float32),
            ] + gain_shapes + [
                sems((2, parts, 2)), sems((2, parts, n)), sems((2, parts, n)), sems((k,)), sems((k,)),
                sems((2, n // 2, 2, parts)), sems((2, n // 2, 2, parts)),
            ]
        results = pl.pallas_call(
            body,
            out_shape=[shaped(*shape) for shape in shapes],
            in_specs=[hbm] * 4 + [small_spec] * 3,
            out_specs=[vmem] * 5,
            scratch_shapes=scratch,
            compiler_params=pltpu.CompilerParams(
                collective_id=0, has_side_effects=True, vmem_limit_bytes=46 * 2**20
            ),
        )(
            one_gate, other_gate, one_up, other_up,
            mix_share.reshape(1, rows), norm_train.reshape(1, piece), norm_step.reshape(1, piece),
        )
        if near:
            results = pl.pallas_call(
                writer,
                out_shape=[jax.ShapeDtypeStruct(*shape) for shape in shapes],
                in_specs=[vmem] * 5,
                out_specs=[hbm] * 5,
                scratch_shapes=[pltpu.SemaphoreType.DMA((11,))],
                compiler_params=pltpu.CompilerParams(vmem_limit_bytes=2**20),
            )(*results)
        final_gate, final_up, column_gate, column_up, serve_norm = results
        return (
            final_gate, final_up, column_gate.reshape(cols), column_up.reshape(cols),
            serve_norm.reshape(n * k * piece),
        )

    return jax.shard_map(
        local,
        mesh=mesh,
        in_specs=(
            P("shard", "model"), P("shard", "model"), P("shard", "model"), P("shard", "model"),
            P("shard"), P(("shard", "model")), P(("shard", "model")),
        ),
        out_specs=(P(None, "model"), P(None, "model"), P("model"), P("model"), P()),
        check_vma=False,
    )
```

```python
import functools

import jax
import jax.numpy as jnp
from jax import lax
from jax.experimental import pallas as pl
from jax.experimental.pallas import tpu as pltpu
from jax.sharding import PartitionSpec as P

MESH = pl.DeviceIdType.MESH
LANES = 128


def position_of(index, n):
    return jnp.where(index % 2 == 0, index // 2, n - 1 - index // 2)


def index_at(position, n):
    return jnp.where(position < n // 2, 2 * position, 2 * (n - 1 - position) + 1)


def kernel(
    n, k, parts,
    one_gate, other_gate, one_up, other_up, mix, norm_train, norm_step,
    final_gate, final_up, column_gate, column_up, serve_norm,
    held_one, held_other, share, maxima, gains, gain_rows,
    load_sem, max_send, max_recv, norm_send, norm_recv, ring_send, ring_recv,
):
    rows, cols = one_gate.shape
    piece = norm_train.shape[1]
    part = cols // parts
    me, col = lax.axis_index("shard"), lax.axis_index("model")
    at = position_of(me, n)

    ones, others = (one_gate, one_up), (other_gate, other_up)
    finals, columns = (final_gate, final_up), (column_gate, column_up)

    loads = {}
    for w in range(2):
        for c in range(parts):
            span = pl.ds(c * part, part)
            pair = (
                pltpu.make_async_copy(ones[w].at[:, span], held_one.at[w, :, span], load_sem.at[w, c, 0]),
                pltpu.make_async_copy(others[w].at[:, span], held_other.at[w, :, span], load_sem.at[w, c, 1]),
            )
            for copy in pair:
                copy.start()
            loads[w, c] = pair

    barrier = pltpu.get_barrier_semaphore()
    for d in range(1, n):
        pl.semaphore_signal(barrier, inc=1, device_id=((me + d) % n, col), device_id_type=MESH)
    for d in range(1, k):
        pl.semaphore_signal(barrier, inc=1, device_id=(me, (col + d) % k), device_id_type=MESH)

    share[...] = jnp.broadcast_to(mix[...], (LANES, rows)).T

    maxima[1, parts - 1, 0, :, part:part + piece] = norm_train[...] + norm_step[...]

    def mixed(w, c):
        for copy in loads[w, c]:
            copy.wait()
        span = pl.ds(c * part, part)

        def step(g, top):
            lines = pl.ds(pl.multiple_of(g * 8, 8), 8)
            m = share[lines, 0:1]
            result = m * held_one[w, lines, span] + (1.0 - m) * held_other[w, lines, span]
            held_one[w, lines, span] = result
            return jnp.maximum(top, jnp.abs(result))

        top = lax.fori_loop(0, rows // 8, step, jnp.zeros((8, part), jnp.float32), unroll=4)
        maxima[w, c, 0, :, 0:part] = jnp.max(top, axis=0, keepdims=True)

    def tell(w, c):
        width = part + LANES if (w, c) == (1, parts - 1) else part
        copies = []
        for d in range(1, n):
            copy = pltpu.make_async_remote_copy(
                src_ref=maxima.at[w, c, 0, :, pl.ds(0, width)], dst_ref=maxima.at[w, c, d, :, pl.ds(0, width)],
                send_sem=max_send.at[w, c, d], recv_sem=max_recv.at[w, c, d],
                device_id=((me + d) % n, col), device_id_type=MESH,
            )
            copy.start()
            copies.append(copy)
        return copies

    def ring(way, hop, w, c):
        origin = index_at((at + (n - hop if way == 0 else hop)) % n, n)
        lines, span = pl.ds(pl.multiple_of(origin * rows, rows), rows), pl.ds(c * part, part)
        to = index_at((at + (1 if way == 0 else n - 1)) % n, n)
        return pltpu.make_async_remote_copy(
            src_ref=finals[w].at[lines, span], dst_ref=finals[w].at[lines, span],
            send_sem=ring_send.at[way, hop, w, c], recv_sem=ring_recv.at[way, hop, w, c],
            device_id=(to, col), device_id_type=MESH,
        )

    def scaled(w, c, inverse):
        span = pl.ds(c * part, part)

        def step(g, _):
            start = pl.multiple_of(g * 16, 16)
            to = pl.multiple_of(me * rows + g * 16, 16)
            finals[w][pl.ds(to, 16), span] = (held_one[w, pl.ds(start, 16), span] * inverse).astype(jnp.bfloat16)
            return 0

        lax.fori_loop(0, rows // 16, step, 0, unroll=2)

    units = [(w, c) for w in range(2) for c in range(parts)]
    told = {}
    for w, c in units:
        mixed(w, c)
        if (w, c) == units[0]:
            pl.semaphore_wait(barrier, n - 1 + k - 1)
        told[w, c] = tell(w, c)

    sent, norms = {}, []
    for w, c in units:
        for copy in told[w, c]:
            copy.wait_recv()
        column = jnp.max(maxima[w, c, :, :, 0:part], axis=0)
        columns[w][:, pl.ds(c * part, part)] = column
        scaled(w, c, 1.0 / column)
        for way in range(2):
            sent[way, 0, w, c] = ring(way, 0, w, c)
            sent[way, 0, w, c].start()

    for d in range(n):
        gains[0, pl.ds((me + (n - d)) % n, 1), :] = maxima[1, parts - 1, d, :, part:part + LANES]
    for d in range(1, k):
        copy = pltpu.make_async_remote_copy(
            src_ref=gains.at[0], dst_ref=gains.at[d],
            send_sem=norm_send.at[d], recv_sem=norm_recv.at[d],
            device_id=(me, (col + d) % k), device_id_type=MESH,
        )
        copy.start()
        norms.append(copy)
    for copy in norms:
        copy.wait_recv()
    gain = jnp.concatenate([gains[(col + (k - j)) % k][:, 0:piece] for j in range(k)], axis=1)
    if serve_norm.shape[1] == gain.shape[1]:
        serve_norm[...] = gain.astype(jnp.bfloat16)
    else:
        each = k * piece // LANES
        for i in range(n * each):
            at_lane = i % each * LANES
            gain_rows[i:i + 1, :] = gain[i // each:i // each + 1, at_lane:at_lane + LANES]
        serve_norm[...] = gain_rows[...].astype(jnp.bfloat16)

    for hop in range(1, n // 2 + 1):
        for w in range(2):
            for c in range(parts):
                for way in range(2):
                    if (way, hop - 1, w, c) not in sent:
                        continue
                    sent[way, hop - 1, w, c].wait_recv()
                    if hop < n // 2 - 1 or (hop == n // 2 - 1 and way == w):
                        sent[way, hop, w, c] = ring(way, hop, w, c)
                        sent[way, hop, w, c].start()

    for copy in sent.values():
        copy.wait_send()
    for copy in sum(told.values(), norms):
        copy.wait_send()


def near_kernel(
    n, k, units, direct, early,
    one_gate, other_gate, one_up, other_up, mix, norm_train, norm_step,
    final_gate, final_up, column_gate, column_up, serve_norm,
    taken, result, mix_held, norm_held, share, raw, mine, heard, partial, whole, gains, gain_rows,
    load_sem, small_sem, raw_sem, max_send, max_recv, part_sem, whole_sem, norm_sem, ring_send, ring_recv,
):
    rows, cols = one_gate.shape
    piece = norm_train.shape[1]
    block = mine.shape[2]
    me, col = lax.axis_index("shard"), lax.axis_index("model")
    at = position_of(me, n)

    ones, others = (one_gate, one_up), (other_gate, other_up)
    finals, columns = (final_gate, final_up), (column_gate, column_up)

    def peer(d):
        return ((me + d) % n, col)

    def wait_for(ref, sem):
        pltpu.make_async_copy(ref, ref, sem).wait()

    def load(u):
        w, first, width = units[u]
        span = pl.ds(first, width)
        for i, source in enumerate((ones[w], others[w])):
            pltpu.make_async_copy(source.at[:, span], taken.at[w, i, :, span], load_sem.at[u]).start()

    pltpu.make_async_copy(mix, mix_held, small_sem.at[0]).start()
    load(0)
    barrier = pltpu.get_barrier_semaphore()
    for d in range(1, n):
        pl.semaphore_signal(barrier, inc=1, device_id=peer(d), device_id_type=MESH)
    for d in range(1, k):
        pl.semaphore_signal(barrier, inc=1, device_id=(me, (col + d) % k), device_id_type=MESH)
    load(early)
    for u in range(1, early):
        load(u)
    for i, source in enumerate((norm_train, norm_step)):
        pltpu.make_async_copy(source, norm_held.at[i], small_sem.at[1]).start()

    wait_for(mix_held, small_sem.at[0])
    share[...] = jnp.broadcast_to(mix_held[...], (LANES, rows)).T

    def mixed(u):
        w, first, width = units[u]
        span = pl.ds(first, width)
        wait_for(taken.at[w, :, :, span], load_sem.at[u])

        def step(g, top):
            lines = pl.ds(pl.multiple_of(g * 8, 8), 8)
            m = share[lines, :]
            both = jnp.concatenate([m] * (width // LANES), axis=1)
            rest = jnp.concatenate([1.0 - m] * (width // LANES), axis=1)
            value = both * taken[w, 0, lines, span] + rest * taken[w, 1, lines, span]
            result[w, lines, span] = value
            return jnp.maximum(top, jnp.abs(value))

        top = lax.fori_loop(0, rows // 8, step, jnp.zeros((8, width), jnp.float32), unroll=4)
        top = jnp.max(top, axis=0, keepdims=True)
        done = 0
        while done < width:
            b, lane = (w * cols + first + done) // block, (first + done) % block
            take = min(block - lane, width - done)
            mine[b, :, lane:lane + take] = top[:, done:done + take]
            done += take

    def tell(u):
        for d in range(1, n):
            pltpu.make_async_remote_copy(
                src_ref=mine.at[u], dst_ref=heard.at[u, d],
                send_sem=max_send.at[0], recv_sem=max_recv.at[u], device_id=peer(d), device_id_type=MESH,
            ).start()

    def heard_of(u):
        wait_for(heard.at[u, pl.ds(1, n - 1)], max_recv.at[u])
        top = mine[u]
        for d in range(1, n):
            top = jnp.maximum(top, heard[u, d])
        return 1.0 / top

    def toward(way):
        return index_at((at + (1 if way == 0 else n - 1)) % n, n)

    def origin_of(way, hop):
        return index_at((at + (n - hop if way == 0 else hop)) % n, n)

    def place(origin, w, first, width):
        return finals[w].at[pl.ds(pl.multiple_of(origin * rows, rows), rows), pl.ds(first, width)]

    def send(way, hop, w, first, width, send_sem, recv_sem):
        part = place(origin_of(way, hop), w, first, width)
        pltpu.make_async_remote_copy(
            src_ref=part, dst_ref=part, send_sem=send_sem, recv_sem=recv_sem,
            device_id=(toward(way), col), device_id_type=MESH,
        ).start()

    e_weight, e_first, e_width = units[early]

    def scaled(u, origin, inverse, read):
        w, first, width = units[u]

        def step(g, _):
            start = pl.multiple_of(g * 16, 16)
            to = pl.multiple_of(origin * rows + g * 16, 16)
            finals[w][pl.ds(to, 16), pl.ds(first, width)] = (read(pl.ds(start, 16)) * inverse).astype(jnp.bfloat16)
            return 0

        lax.fori_loop(0, rows // 16, step, 0, unroll=2)

    def held(u):
        w, first, width = units[u]
        return lambda lines: result[w, lines, pl.ds(first, width)]

    def begin(u, inverse):
        scaled(u, me, inverse, held(u))
        for way in range(2):
            send(way, 0, *units[u], ring_send.at[way, units[u][0]], ring_recv.at[0, way, units[u][0]])

    mixed(0)
    pl.semaphore_wait(barrier, n - 1 + k - 1)
    tell(0)
    mixed(early)
    for way in range(2):
        pltpu.make_async_remote_copy(
            src_ref=result.at[e_weight, :, pl.ds(e_first, e_width)], dst_ref=raw.at[way],
            send_sem=raw_sem.at[0], recv_sem=raw_sem.at[1], device_id=(toward(way), col), device_id_type=MESH,
        ).start()
    for u in range(1, direct):
        mixed(u)
        tell(u)
    for u in range(direct, early):
        mixed(u)
    for d in range(1, n):
        pltpu.make_async_remote_copy(
            src_ref=mine.at[(me + d) % n], dst_ref=partial.at[d],
            send_sem=part_sem.at[0], recv_sem=part_sem.at[1], device_id=peer(d), device_id_type=MESH,
        ).start()
    wait_for(norm_held, small_sem.at[1])

    begin(0, heard_of(0))

    wait_for(partial.at[pl.ds(1, n - 1)], part_sem.at[1])
    top = mine[me]
    for d in range(1, n):
        top = jnp.maximum(top, partial[d])
    whole[me, :, 0:block] = top
    whole[me, :, block:block + piece] = norm_held[0] + norm_held[1]
    for d in range(1, n):
        pltpu.make_async_remote_copy(
            src_ref=whole.at[me], dst_ref=whole.at[me],
            send_sem=whole_sem.at[0], recv_sem=whole_sem.at[1], device_id=peer(d), device_id_type=MESH,
        ).start()

    for u in range(1, direct):
        begin(u, heard_of(u))

    wait_for(whole.at[pl.ds(1, n - 1)], whole_sem.at[1])
    for b in range(n):
        w, first = b * block // cols, b * block % cols
        columns[w][:, first:first + block] = whole[b, :, 0:block]

    for u in range(direct, early):
        w, first, width = units[u]
        begin(u, 1.0 / columns[w][:, first:first + width])

    inverse = 1.0 / columns[e_weight][:, e_first:e_first + e_width]
    wait_for(raw, raw_sem.at[1])
    for way in range(2):
        scaled(early, origin_of(way, 1), inverse, lambda lines: raw[way, lines, :])
    scaled(early, me, inverse, held(early))

    for d in range(n):
        gains[0, d:d + 1, :] = whole[d, :, block:block + LANES]
    for d in range(1, k):
        pltpu.make_async_remote_copy(
            src_ref=gains.at[0], dst_ref=gains.at[d], send_sem=norm_sem.at[0], recv_sem=norm_sem.at[1],
            device_id=(me, (col + d) % k), device_id_type=MESH,
        ).start()
    wait_for(gains.at[pl.ds(1, k - 1)], norm_sem.at[1])
    gain = jnp.concatenate([gains[(col + (k - j)) % k][:, 0:piece] for j in range(k)], axis=1)
    if serve_norm.shape[1] == gain.shape[1]:
        serve_norm[...] = gain.astype(jnp.bfloat16)
    else:
        each = k * piece // LANES
        for i in range(n * each):
            at_lane = i % each * LANES
            gain_rows[i:i + 1, :] = gain[i // each:i // each + 1, at_lane:at_lane + LANES]
        serve_norm[...] = gain_rows[...].astype(jnp.bfloat16)

    last = n // 2 - 1
    halves = ((0, cols // 2, ring_recv.at[last - 1, 1, 1]), (cols // 2, cols // 2, ring_recv.at[last, 0, 1]))

    for hop in range(1, last + 1):
        for w in range(2):
            for way in range(2):
                split = (way, w) == (1, 1)
                width = e_first if (hop, w) == (1, e_weight) else cols
                if hop == last and split:
                    for first, half, sem in halves:
                        wait_for(place(origin_of(way, hop), w, first, half), sem)
                        send(way, hop, w, first, half, ring_send.at[2, 0], ring_recv.at[hop, way, w])
                elif hop < last or way == w:
                    wait_for(place(origin_of(way, hop), w, 0, width), ring_recv.at[hop - 1, way, w])
                    wait_for(place(me, w, 0, width), ring_send.at[way, w])
                    if hop == last - 1 and split:
                        for first, half, sem in halves:
                            send(way, hop, w, first, half, ring_send.at[way, w], sem)
                    else:
                        send(way, hop, w, 0, cols, ring_send.at[way, w], ring_recv.at[hop, way, w])

    for way in range(2):
        wait_for(place(origin_of(way, last), 1 - way, 0, cols), ring_recv.at[last - 1, way, 1 - way])
    for way in range(2):
        wait_for(place(origin_of(way, last + 1), way, 0, cols), ring_recv.at[last, way, way])
    for way in range(2):
        for w in range(2):
            wait_for(place(me, w, 0, cols), ring_send.at[way, w])
    wait_for(place(me, 1, 0, cols), ring_send.at[2, 0])
    wait_for(raw, raw_sem.at[0])
    wait_for(heard.at[:, pl.ds(1, n - 1)], max_send.at[0])
    wait_for(partial.at[pl.ds(1, n - 1)], part_sem.at[0])
    wait_for(whole.at[pl.ds(1, n - 1)], whole_sem.at[0])
    wait_for(gains.at[pl.ds(1, k - 1)], norm_sem.at[0])


def writer(*refs):
    (sem,), count = refs[-1:], (len(refs) - 1) // 2
    pairs = list(zip(refs[:count], refs[count:-1]))
    for i, (source, target) in enumerate(pairs):
        pieces = 4 if source.shape[0] > LANES else 1
        lines = source.shape[0] // pieces
        for p in range(pieces):
            span = pl.ds(p * lines, lines)
            pltpu.make_async_copy(source.at[span], target.at[span], sem.at[i]).start()
    for i, (source, target) in enumerate(pairs):
        pltpu.make_async_copy(source, target, sem.at[i]).wait()


def solution(mesh):
    n, k = mesh.shape["shard"], mesh.shape["model"]

    def local(one_gate, other_gate, one_up, other_up, mix_share, norm_train, norm_step):
        rows, cols = one_gate.shape
        piece = norm_train.shape[0]
        parts = 2 if n <= 8 else 1
        near = 4 < n <= 8
        shaped = pltpu.VMEM if near else jax.ShapeDtypeStruct
        norm_shape = (n * k * piece // LANES, LANES) if k * piece % LANES == 0 else (n, k * piece)
        shapes = [
            ((n * rows, cols), jnp.bfloat16), ((n * rows, cols), jnp.bfloat16),
            ((1, cols), jnp.float32), ((1, cols), jnp.float32), (norm_shape, jnp.bfloat16),
        ]
        hbm, vmem = pl.BlockSpec(memory_space=pltpu.HBM), pl.BlockSpec(memory_space=pltpu.VMEM)
        block = 2 * cols // n
        e = cols // 16
        units = (
            (0, 0, block), (0, block, block), (0, 2 * block, cols - 2 * block),
            (1, 0, 8 * e), (1, 8 * e, 7 * e), (1, 15 * e, e),
        )
        direct, early = 2, len(units) - 1
        gain_shapes = [
            pltpu.VMEM((k, n, LANES), jnp.float32),
            pltpu.VMEM((max(n * k * piece // LANES, 8), LANES), jnp.float32),
        ]
        sems = pltpu.SemaphoreType.DMA
        if near:
            body = functools.partial(near_kernel, n, k, units, direct, early)
            small_spec = hbm
            scratch = [
                pltpu.VMEM((2, 2, rows, cols), jnp.float32),
                pltpu.VMEM((2, rows, cols), jnp.float32),
                pltpu.VMEM((1, rows), jnp.float32), pltpu.VMEM((2, 1, piece), jnp.float32),
                pltpu.VMEM((rows, LANES), jnp.float32),
                pltpu.VMEM((2, rows, e), jnp.float32),
                pltpu.VMEM((n, 1, block), jnp.float32),
                pltpu.VMEM((direct, n, 1, block), jnp.float32),
                pltpu.VMEM((n, 1, block), jnp.float32),
                pltpu.VMEM((n, 1, block + LANES), jnp.float32),
            ] + gain_shapes + [
                sems((len(units),)), sems((2,)), sems((2,)), sems((1,)), sems((direct,)), sems((2,)), sems((2,)), sems((2,)),
                sems((3, 2)), sems((n // 2, 2, 2)),
            ]
        else:
            body = functools.partial(kernel, n, k, parts)
            small_spec = vmem
            scratch = [pltpu.VMEM((2, rows, cols), jnp.float32)] * 2 + [
                pltpu.VMEM((rows, LANES), jnp.float32),
                pltpu.VMEM((2, parts, n, 1, cols // parts + LANES), jnp.float32),
            ] + gain_shapes + [
                sems((2, parts, 2)), sems((2, parts, n)), sems((2, parts, n)), sems((k,)), sems((k,)),
                sems((2, n // 2, 2, parts)), sems((2, n // 2, 2, parts)),
            ]
        results = pl.pallas_call(
            body,
            out_shape=[shaped(*shape) for shape in shapes],
            in_specs=[hbm] * 4 + [small_spec] * 3,
            out_specs=[vmem] * 5,
            scratch_shapes=scratch,
            compiler_params=pltpu.CompilerParams(
                collective_id=0, has_side_effects=True, vmem_limit_bytes=46 * 2**20
            ),
        )(
            one_gate, other_gate, one_up, other_up,
            mix_share.reshape(1, rows), norm_train.reshape(1, piece), norm_step.reshape(1, piece),
        )
        if near:
            results = pl.pallas_call(
                writer,
                out_shape=[jax.ShapeDtypeStruct(*shape) for shape in shapes],
                in_specs=[vmem] * 5,
                out_specs=[hbm] * 5,
                scratch_shapes=[pltpu.SemaphoreType.DMA((5,))],
                compiler_params=pltpu.CompilerParams(vmem_limit_bytes=2**20),
            )(*results)
        final_gate, final_up, column_gate, column_up, serve_norm = results
        return (
            final_gate, final_up, column_gate.reshape(cols), column_up.reshape(cols),
            serve_norm.reshape(n * k * piece),
        )

    return jax.shard_map(
        local,
        mesh=mesh,
        in_specs=(
            P("shard", "model"), P("shard", "model"), P("shard", "model"), P("shard", "model"),
            P("shard"), P(("shard", "model")), P(("shard", "model")),
        ),
        out_specs=(P(None, "model"), P(None, "model"), P("model"), P("model"), P()),
        check_vma=False,
    )
```

```python
import functools

import jax
import jax.numpy as jnp
from jax import lax
from jax.experimental import pallas as pl
from jax.experimental.pallas import tpu as pltpu
from jax.sharding import PartitionSpec as P

MESH = pl.DeviceIdType.MESH
LANES = 128


def position_of(index, n):
    return jnp.where(index % 2 == 0, index // 2, n - 1 - index // 2)


def index_at(position, n):
    return jnp.where(position < n // 2, 2 * position, 2 * (n - 1 - position) + 1)


def kernel(
    n, k, parts,
    one_gate, other_gate, one_up, other_up, mix, norm_train, norm_step,
    final_gate, final_up, column_gate, column_up, serve_norm,
    held_one, held_other, share, maxima, gains, gain_rows,
    load_sem, max_send, max_recv, norm_send, norm_recv, ring_send, ring_recv,
):
    rows, cols = one_gate.shape
    piece = norm_train.shape[1]
    part = cols // parts
    me, col = lax.axis_index("shard"), lax.axis_index("model")
    at = position_of(me, n)

    ones, others = (one_gate, one_up), (other_gate, other_up)
    finals, columns = (final_gate, final_up), (column_gate, column_up)

    loads = {}
    for w in range(2):
        for c in range(parts):
            span = pl.ds(c * part, part)
            pair = (
                pltpu.make_async_copy(ones[w].at[:, span], held_one.at[w, :, span], load_sem.at[w, c, 0]),
                pltpu.make_async_copy(others[w].at[:, span], held_other.at[w, :, span], load_sem.at[w, c, 1]),
            )
            for copy in pair:
                copy.start()
            loads[w, c] = pair

    barrier = pltpu.get_barrier_semaphore()
    for d in range(1, n):
        pl.semaphore_signal(barrier, inc=1, device_id=((me + d) % n, col), device_id_type=MESH)
    for d in range(1, k):
        pl.semaphore_signal(barrier, inc=1, device_id=(me, (col + d) % k), device_id_type=MESH)

    share[...] = jnp.broadcast_to(mix[...], (LANES, rows)).T

    maxima[1, parts - 1, 0, :, part:part + piece] = norm_train[...] + norm_step[...]

    def mixed(w, c):
        for copy in loads[w, c]:
            copy.wait()
        span = pl.ds(c * part, part)

        def step(g, top):
            lines = pl.ds(pl.multiple_of(g * 8, 8), 8)
            m = share[lines, 0:1]
            result = m * held_one[w, lines, span] + (1.0 - m) * held_other[w, lines, span]
            held_one[w, lines, span] = result
            return jnp.maximum(top, jnp.abs(result))

        top = lax.fori_loop(0, rows // 8, step, jnp.zeros((8, part), jnp.float32), unroll=4)
        maxima[w, c, 0, :, 0:part] = jnp.max(top, axis=0, keepdims=True)

    def tell(w, c):
        width = part + LANES if (w, c) == (1, parts - 1) else part
        copies = []
        for d in range(1, n):
            copy = pltpu.make_async_remote_copy(
                src_ref=maxima.at[w, c, 0, :, pl.ds(0, width)], dst_ref=maxima.at[w, c, d, :, pl.ds(0, width)],
                send_sem=max_send.at[w, c, d], recv_sem=max_recv.at[w, c, d],
                device_id=((me + d) % n, col), device_id_type=MESH,
            )
            copy.start()
            copies.append(copy)
        return copies

    def ring(way, hop, w, c):
        origin = index_at((at + (n - hop if way == 0 else hop)) % n, n)
        lines, span = pl.ds(pl.multiple_of(origin * rows, rows), rows), pl.ds(c * part, part)
        to = index_at((at + (1 if way == 0 else n - 1)) % n, n)
        return pltpu.make_async_remote_copy(
            src_ref=finals[w].at[lines, span], dst_ref=finals[w].at[lines, span],
            send_sem=ring_send.at[way, hop, w, c], recv_sem=ring_recv.at[way, hop, w, c],
            device_id=(to, col), device_id_type=MESH,
        )

    def scaled(w, c, inverse):
        span = pl.ds(c * part, part)

        def step(g, _):
            start = pl.multiple_of(g * 16, 16)
            to = pl.multiple_of(me * rows + g * 16, 16)
            finals[w][pl.ds(to, 16), span] = (held_one[w, pl.ds(start, 16), span] * inverse).astype(jnp.bfloat16)
            return 0

        lax.fori_loop(0, rows // 16, step, 0, unroll=2)

    units = [(w, c) for w in range(2) for c in range(parts)]
    told = {}
    for w, c in units:
        mixed(w, c)
        if (w, c) == units[0]:
            pl.semaphore_wait(barrier, n - 1 + k - 1)
        told[w, c] = tell(w, c)

    sent, norms = {}, []
    for w, c in units:
        for copy in told[w, c]:
            copy.wait_recv()
        column = jnp.max(maxima[w, c, :, :, 0:part], axis=0)
        columns[w][:, pl.ds(c * part, part)] = column
        scaled(w, c, 1.0 / column)
        for way in range(2):
            sent[way, 0, w, c] = ring(way, 0, w, c)
            sent[way, 0, w, c].start()

    for d in range(n):
        gains[0, pl.ds((me + (n - d)) % n, 1), :] = maxima[1, parts - 1, d, :, part:part + LANES]
    for d in range(1, k):
        copy = pltpu.make_async_remote_copy(
            src_ref=gains.at[0], dst_ref=gains.at[d],
            send_sem=norm_send.at[d], recv_sem=norm_recv.at[d],
            device_id=(me, (col + d) % k), device_id_type=MESH,
        )
        copy.start()
        norms.append(copy)
    for copy in norms:
        copy.wait_recv()
    gain = jnp.concatenate([gains[(col + (k - j)) % k][:, 0:piece] for j in range(k)], axis=1)
    if serve_norm.shape[1] == gain.shape[1]:
        serve_norm[...] = gain.astype(jnp.bfloat16)
    else:
        each = k * piece // LANES
        for i in range(n * each):
            at_lane = i % each * LANES
            gain_rows[i:i + 1, :] = gain[i // each:i // each + 1, at_lane:at_lane + LANES]
        serve_norm[...] = gain_rows[...].astype(jnp.bfloat16)

    for hop in range(1, n // 2 + 1):
        for w in range(2):
            for c in range(parts):
                for way in range(2):
                    if (way, hop - 1, w, c) not in sent:
                        continue
                    sent[way, hop - 1, w, c].wait_recv()
                    if hop < n // 2 - 1 or (hop == n // 2 - 1 and way == w):
                        sent[way, hop, w, c] = ring(way, hop, w, c)
                        sent[way, hop, w, c].start()

    for copy in sent.values():
        copy.wait_send()
    for copy in sum(told.values(), norms):
        copy.wait_send()


class Ring:
    def __init__(self, n, rows, blocks, sends, recvs):
        self.n, self.rows, self.blocks, self.sends, self.recvs = n, rows, blocks, sends, recvs
        self.me, self.col = lax.axis_index("shard"), lax.axis_index("model")
        self.at = position_of(self.me, n)

    def toward(self, way):
        return index_at((self.at + (1 if way == 0 else self.n - 1)) % self.n, self.n)

    def origin_of(self, way, hop):
        return index_at((self.at + (self.n - hop if way == 0 else hop)) % self.n, self.n)

    def place(self, b, origin, first, width):
        ref, start = self.blocks[b][0:2]
        lines = pl.ds(pl.multiple_of(origin * self.rows, self.rows), self.rows)
        return ref.at[lines, pl.ds(start + first, width)]

    def send(self, way, hop, b, first, width, source=None):
        part = self.place(b, self.origin_of(way, hop), first, width)
        pltpu.make_async_remote_copy(
            src_ref=part if source is None else source, dst_ref=part,
            send_sem=self.sends.at[way, b], recv_sem=self.recvs.at[hop, way, b],
            device_id=(self.toward(way), self.col), device_id_type=MESH,
        ).start()

    def arrived(self, way, hop, b, first, width):
        wait_for(self.place(b, self.origin_of(way, hop + 1), first, width), self.recvs.at[hop, way, b])

    def final_part(self, way, b):
        width = self.blocks[b][2]
        if b < 2:
            return (0, width) if way == b else None
        return (way * (width // 2), width // 2)

    def each(self, act):
        for i in range(len(self.blocks)):
            for way in range(2):
                b = (i, 1 - i if i < 2 else i)[way]
                only = self.blocks[b][4]
                if only is None:
                    act(way, b)
                else:
                    pl.when(only)(functools.partial(act, way, b))

    def go(self):
        last = self.n // 2 - 1
        for hop in range(1, last + 1):
            def forward(way, b, hop=hop):
                width = self.blocks[b][3 if hop == 1 else 2]
                part = (0, self.blocks[b][2]) if hop < last else self.final_part(way, b)
                if part is not None:
                    self.arrived(way, hop - 1, b, 0, width)
                    wait_for(self.place(b, self.me, 0, width), self.sends.at[way, b])
                    self.send(way, hop, b, *part)
            self.each(forward)

        def rest(way, b):
            if self.final_part(way, b) is None:
                self.arrived(way, last - 1, b, 0, self.blocks[b][2])

        def end(way, b):
            part = self.final_part(way, b)
            if part is not None:
                self.arrived(way, last, b, *part)

        def drain(way, b):
            part = self.final_part(way, b) or (0, self.blocks[b][2])
            wait_for(self.place(b, self.me, *part), self.sends.at[way, b])

        for act in (rest, end, drain):
            self.each(act)


def wait_for(ref, sem):
    pltpu.make_async_copy(ref, ref, sem).wait()


def near_kernel(
    n, k, units, direct, early,
    one_gate, other_gate, one_up, other_up, mix, norm_train, norm_step,
    final_gate, column_gate, column_up, serve_norm, own_up, extra,
    taken, result, mix_held, norm_held, share, raw, mine, heard, partial, whole, gains, gain_rows,
    load_sem, small_sem, raw_sem, max_send, max_recv, part_sem, whole_sem, norm_sem, ring_send, ring_recv,
):
    rows, cols = one_gate.shape
    piece = norm_train.shape[1]
    block = mine.shape[2]
    me, col = lax.axis_index("shard"), lax.axis_index("model")

    ones, others = (one_gate, one_up), (other_gate, other_up)
    columns = (column_gate, column_up)
    odd = col % 2 == 1

    def peer(d):
        return ((me + d) % n, col)

    def load(u):
        w, first, width = units[u]
        span = pl.ds(first, width)
        for i, source in enumerate((ones[w], others[w])):
            pltpu.make_async_copy(source.at[:, span], taken.at[w, i, :, span], load_sem.at[u]).start()

    pltpu.make_async_copy(mix, mix_held, small_sem.at[0]).start()
    load(0)
    barrier = pltpu.get_barrier_semaphore()
    for d in range(1, n):
        pl.semaphore_signal(barrier, inc=1, device_id=peer(d), device_id_type=MESH)
    for d in range(1, k):
        pl.semaphore_signal(barrier, inc=1, device_id=(me, (col + d) % k), device_id_type=MESH)
    load(early)
    for u in range(1, early):
        load(u)
    for i, source in enumerate((norm_train, norm_step)):
        pltpu.make_async_copy(source, norm_held.at[i], small_sem.at[1]).start()

    wait_for(mix_held, small_sem.at[0])
    share[...] = jnp.broadcast_to(mix_held[...], (LANES, rows)).T

    def mixed(u):
        w, first, width = units[u]
        span = pl.ds(first, width)
        wait_for(taken.at[w, :, :, span], load_sem.at[u])

        def step(g, top):
            lines = pl.ds(pl.multiple_of(g * 8, 8), 8)
            m = share[lines, :]
            both = jnp.concatenate([m] * (width // LANES), axis=1)
            rest = jnp.concatenate([1.0 - m] * (width // LANES), axis=1)
            value = both * taken[w, 0, lines, span] + rest * taken[w, 1, lines, span]
            result[w, lines, span] = value
            return jnp.maximum(top, jnp.abs(value))

        top = lax.fori_loop(0, rows // 8, step, jnp.zeros((8, width), jnp.float32), unroll=4)
        top = jnp.max(top, axis=0, keepdims=True)
        done = 0
        while done < width:
            b, lane = (w * cols + first + done) // block, (first + done) % block
            take = min(block - lane, width - done)
            mine[b, :, lane:lane + take] = top[:, done:done + take]
            done += take

    def tell(u):
        for d in range(1, n):
            pltpu.make_async_remote_copy(
                src_ref=mine.at[u], dst_ref=heard.at[u, d],
                send_sem=max_send.at[0], recv_sem=max_recv.at[u], device_id=peer(d), device_id_type=MESH,
            ).start()

    def heard_of(u):
        wait_for(heard.at[u, pl.ds(1, n - 1)], max_recv.at[u])
        top = mine[u]
        for d in range(1, n):
            top = jnp.maximum(top, heard[u, d])
        return 1.0 / top

    e_weight, e_first, e_width = units[early]
    half = cols // 2
    shared = extra.shape[1]
    ring = Ring(
        n, rows,
        (
            (final_gate, 0, half, half, None), (final_gate, half, half, half - e_width, None),
            (extra, 0, shared, shared, odd),
        ),
        ring_send, ring_recv,
    )

    def scaled(target, origin, first, width, inverse, read):
        def step(g, _):
            start = pl.multiple_of(g * 16, 16)
            to = pl.multiple_of(origin * rows + g * 16, 16)
            target[pl.ds(to, 16), pl.ds(first, width)] = (read(pl.ds(start, 16)) * inverse).astype(jnp.bfloat16)
            return 0

        lax.fori_loop(0, rows // 16, step, 0, unroll=2)

    def held(w, first, width):
        return lambda lines: result[w, lines, pl.ds(first, width)]

    def begin(u, inverse):
        w, first, width = units[u]
        scaled(final_gate, me, first, width, inverse, held(w, first, width))
        for way in range(2):
            b = first // half
            ring.send(way, 0, b, first - b * half, width)

    mixed(0)
    pl.semaphore_wait(barrier, n - 1 + k - 1)
    tell(0)
    mixed(early)
    for way in range(2):
        pltpu.make_async_remote_copy(
            src_ref=result.at[e_weight, :, pl.ds(e_first, e_width)], dst_ref=raw.at[way],
            send_sem=raw_sem.at[0], recv_sem=raw_sem.at[1], device_id=(ring.toward(way), col), device_id_type=MESH,
        ).start()
    for u in range(1, direct):
        mixed(u)
        tell(u)
    for u in range(direct, early):
        mixed(u)
    for d in range(1, n):
        pltpu.make_async_remote_copy(
            src_ref=mine.at[(me + d) % n], dst_ref=partial.at[d],
            send_sem=part_sem.at[0], recv_sem=part_sem.at[1], device_id=peer(d), device_id_type=MESH,
        ).start()
    wait_for(norm_held, small_sem.at[1])

    begin(0, heard_of(0))

    wait_for(partial.at[pl.ds(1, n - 1)], part_sem.at[1])
    top = mine[me]
    for d in range(1, n):
        top = jnp.maximum(top, partial[d])
    whole[me, :, 0:block] = top
    whole[me, :, block:block + piece] = norm_held[0] + norm_held[1]
    for d in range(1, n):
        pltpu.make_async_remote_copy(
            src_ref=whole.at[me], dst_ref=whole.at[me],
            send_sem=whole_sem.at[0], recv_sem=whole_sem.at[1], device_id=peer(d), device_id_type=MESH,
        ).start()

    for u in range(1, direct):
        begin(u, heard_of(u))

    wait_for(whole.at[pl.ds(1, n - 1)], whole_sem.at[1])
    for b in range(n):
        w, first = b * block // cols, b * block % cols
        columns[w][:, first:first + block] = whole[b, :, 0:block]

    for u in range(direct, early):
        w, first, width = units[u]
        if w == 0:
            begin(u, 1.0 / columns[0][:, first:first + width])

    inverse_up = 1.0 / columns[1][...]
    scaled(own_up, 0, 0, cols, inverse_up, held(1, 0, cols))

    @pl.when(odd)
    def _():
        scaled(extra, me, 0, shared, inverse_up[:, 0:shared], held(1, 0, shared))
        for way in range(2):
            ring.send(way, 0, 2, 0, shared, own_up.at[:, pl.ds(0, shared)])

    inverse = 1.0 / columns[e_weight][:, e_first:e_first + e_width]
    wait_for(raw, raw_sem.at[1])
    for way in range(2):
        scaled(final_gate, ring.origin_of(way, 1), e_first, e_width, inverse, lambda lines: raw[way, lines, :])
    scaled(final_gate, me, e_first, e_width, inverse, held(e_weight, e_first, e_width))

    for d in range(n):
        gains[0, d:d + 1, :] = whole[d, :, block:block + LANES]
    for d in range(1, k):
        pltpu.make_async_remote_copy(
            src_ref=gains.at[0], dst_ref=gains.at[d], send_sem=norm_sem.at[0], recv_sem=norm_sem.at[1],
            device_id=(me, (col + d) % k), device_id_type=MESH,
        ).start()
    wait_for(gains.at[pl.ds(1, k - 1)], norm_sem.at[1])
    gain = jnp.concatenate([gains[(col + (k - j)) % k][:, 0:piece] for j in range(k)], axis=1)
    if serve_norm.shape[1] == gain.shape[1]:
        serve_norm[...] = gain.astype(jnp.bfloat16)
    else:
        each = k * piece // LANES
        for i in range(n * each):
            at_lane = i % each * LANES
            gain_rows[i:i + 1, :] = gain[i // each:i // each + 1, at_lane:at_lane + LANES]
        serve_norm[...] = gain_rows[...].astype(jnp.bfloat16)

    ring.go()
    wait_for(raw, raw_sem.at[0])
    wait_for(heard.at[:, pl.ds(1, n - 1)], max_send.at[0])
    wait_for(partial.at[pl.ds(1, n - 1)], part_sem.at[0])
    wait_for(whole.at[pl.ds(1, n - 1)], whole_sem.at[0])
    wait_for(gains.at[pl.ds(1, k - 1)], norm_sem.at[0])


def second_kernel(n, own_up, extra, after, final_up, ring_send, ring_recv):
    rows, cols = own_up.shape
    shared = extra.shape[1]
    half = (cols - shared) // 2
    even = lax.axis_index("model") % 2 == 0
    ring = Ring(
        n, rows,
        (
            (final_up, shared, half, half, None), (final_up, shared + half, half, half, None),
            (final_up, 0, shared, shared, even),
        ),
        ring_send, ring_recv,
    )
    barrier = pltpu.get_barrier_semaphore()
    for way in range(2):
        pl.semaphore_signal(barrier, inc=1, device_id=(ring.toward(way), ring.col), device_id_type=MESH)
    pl.semaphore_wait(barrier, 2)

    def first_hop(way, b):
        _, start, width, _, _ = ring.blocks[b]
        ring.send(way, 0, b, 0, width, own_up.at[:, pl.ds(start, width)])

    ring.each(first_hop)

    def copied(source, to, first, width, lines):
        def step(g, _):
            start = pl.multiple_of(g * 16, 16)
            final_up[pl.ds(pl.multiple_of(to + start, 16), 16), pl.ds(first, width)] = source[pl.ds(start, 16), pl.ds(first, width)]
            return 0

        lax.fori_loop(0, lines // 16, step, 0, unroll=2)

    copied(own_up, ring.me * rows, shared, cols - shared, rows)

    @pl.when(even)
    def _():
        copied(own_up, ring.me * rows, 0, shared, rows)

    @pl.when(jnp.logical_not(even))
    def _():
        copied(extra, 0, 0, shared, n * rows)

    ring.go()


def writer(count, *refs):
    sem = refs[-1]
    pairs = list(zip(refs[:count], refs[count:2 * count]))
    for i, (source, target) in enumerate(pairs):
        pieces = 4 if source.shape[0] > LANES else 1
        lines = source.shape[0] // pieces
        for p in range(pieces):
            span = pl.ds(p * lines, lines)
            pltpu.make_async_copy(source.at[span], target.at[span], sem.at[i]).start()
    for after in refs[2 * count:-1]:
        after[...] = jnp.zeros_like(after)
    for i, (source, target) in enumerate(pairs):
        pltpu.make_async_copy(source, target, sem.at[i]).wait()


def solution(mesh):
    n, k = mesh.shape["shard"], mesh.shape["model"]

    def local(one_gate, other_gate, one_up, other_up, mix_share, norm_train, norm_step):
        rows, cols = one_gate.shape
        piece = norm_train.shape[0]
        parts = 2 if n <= 8 else 1
        near = 4 < n <= 8
        norm_shape = (n * k * piece // LANES, LANES) if k * piece % LANES == 0 else (n, k * piece)
        shapes = [
            ((n * rows, cols), jnp.bfloat16), ((n * rows, cols), jnp.bfloat16),
            ((1, cols), jnp.float32), ((1, cols), jnp.float32), (norm_shape, jnp.bfloat16),
        ]
        hbm, vmem = pl.BlockSpec(memory_space=pltpu.HBM), pl.BlockSpec(memory_space=pltpu.VMEM)
        sems = pltpu.SemaphoreType.DMA
        gain_shapes = [
            pltpu.VMEM((k, n, LANES), jnp.float32),
            pltpu.VMEM((max(n * k * piece // LANES, 8), LANES), jnp.float32),
        ]
        operands = (
            one_gate, other_gate, one_up, other_up,
            mix_share.reshape(1, rows), norm_train.reshape(1, piece), norm_step.reshape(1, piece),
        )

        def written(arrays, order):
            count = len(arrays)
            return pl.pallas_call(
                functools.partial(writer, count),
                out_shape=[jax.ShapeDtypeStruct(x.shape, x.dtype) for x in arrays] + [pltpu.VMEM((8, LANES), jnp.float32)] * order,
                in_specs=[vmem] * count,
                out_specs=[hbm] * count + [vmem] * order,
                scratch_shapes=[sems((count,))],
                compiler_params=pltpu.CompilerParams(vmem_limit_bytes=2**20),
            )(*arrays)

        if near:
            block = 2 * cols // n
            e = cols // 16
            shared = cols * 3 // 8
            units = (
                (0, 0, block), (0, block, block), (0, 8 * e, 7 * e),
                (1, 0, 8 * e), (1, 8 * e, 8 * e), (0, 15 * e, e),
            )
            direct, early = 2, len(units) - 1
            final_gate, column_gate, column_up, serve_norm, own_up, extra = pl.pallas_call(
                functools.partial(near_kernel, n, k, units, direct, early),
                out_shape=[pltpu.VMEM(*shape) for shape in shapes[0:1] + shapes[2:5]] + [
                    pltpu.VMEM((rows, cols), jnp.bfloat16), pltpu.VMEM((n * rows, shared), jnp.bfloat16),
                ],
                in_specs=[hbm] * 7,
                out_specs=[vmem] * 6,
                scratch_shapes=[
                    pltpu.VMEM((2, 2, rows, cols), jnp.float32),
                    pltpu.VMEM((2, rows, cols), jnp.float32),
                    pltpu.VMEM((1, rows), jnp.float32), pltpu.VMEM((2, 1, piece), jnp.float32),
                    pltpu.VMEM((rows, LANES), jnp.float32),
                    pltpu.VMEM((2, rows, e), jnp.float32),
                    pltpu.VMEM((n, 1, block), jnp.float32),
                    pltpu.VMEM((direct, n, 1, block), jnp.float32),
                    pltpu.VMEM((n, 1, block), jnp.float32),
                    pltpu.VMEM((n, 1, block + LANES), jnp.float32),
                ] + gain_shapes + [
                    sems((len(units),)), sems((2,)), sems((2,)), sems((1,)), sems((direct,)), sems((2,)), sems((2,)), sems((2,)),
                    sems((2, 3)), sems((n // 2, 2, 3)),
                ],
                compiler_params=pltpu.CompilerParams(collective_id=0, has_side_effects=True, vmem_limit_bytes=51 * 2**20),
            )(*operands)
            final_gate, column_gate, column_up, serve_norm, after = written((final_gate, column_gate, column_up, serve_norm), 1)
            final_up = pl.pallas_call(
                functools.partial(second_kernel, n),
                out_shape=pltpu.VMEM(*shapes[1]),
                in_specs=[vmem] * 3,
                out_specs=vmem,
                scratch_shapes=[sems((2, 3)), sems((n // 2, 2, 3))],
                compiler_params=pltpu.CompilerParams(collective_id=1, has_side_effects=True, vmem_limit_bytes=2**20),
            )(own_up, extra, after)
            (final_up,) = written((final_up,), 0)
        else:
            final_gate, final_up, column_gate, column_up, serve_norm = pl.pallas_call(
                functools.partial(kernel, n, k, parts),
                out_shape=[jax.ShapeDtypeStruct(*shape) for shape in shapes],
                in_specs=[hbm] * 4 + [vmem] * 3,
                out_specs=[vmem] * 5,
                scratch_shapes=[pltpu.VMEM((2, rows, cols), jnp.float32)] * 2 + [
                    pltpu.VMEM((rows, LANES), jnp.float32),
                    pltpu.VMEM((2, parts, n, 1, cols // parts + LANES), jnp.float32),
                ] + gain_shapes + [
                    sems((2, parts, 2)), sems((2, parts, n)), sems((2, parts, n)), sems((k,)), sems((k,)),
                    sems((2, n // 2, 2, parts)), sems((2, n // 2, 2, parts)),
                ],
                compiler_params=pltpu.CompilerParams(collective_id=0, has_side_effects=True, vmem_limit_bytes=46 * 2**20),
            )(*operands)
        return (
            final_gate, final_up, column_gate.reshape(cols), column_up.reshape(cols),
            serve_norm.reshape(n * k * piece),
        )

    return jax.shard_map(
        local,
        mesh=mesh,
        in_specs=(
            P("shard", "model"), P("shard", "model"), P("shard", "model"), P("shard", "model"),
            P("shard"), P(("shard", "model")), P(("shard", "model")),
        ),
        out_specs=(P(None, "model"), P(None, "model"), P("model"), P("model"), P()),
        check_vma=False,
    )
```

```python
import functools

import jax
import jax.numpy as jnp
from jax import lax
from jax.experimental import pallas as pl
from jax.experimental.pallas import tpu as pltpu
from jax.sharding import PartitionSpec as P

MESH = pl.DeviceIdType.MESH
LANES = 128
SHARED = 5
LEADER = 0
PIECES = 8


def position_of(index, n):
    return jnp.where(index % 2 == 0, index // 2, n - 1 - index // 2)


def index_at(position, n):
    return jnp.where(position < n // 2, 2 * position, 2 * (n - 1 - position) + 1)


def kernel(
    n, k, parts,
    one_gate, other_gate, one_up, other_up, mix, norm_train, norm_step,
    final_gate, final_up, column_gate, column_up, serve_norm,
    held_one, held_other, share, maxima, gains, gain_rows,
    load_sem, max_send, max_recv, norm_send, norm_recv, ring_send, ring_recv,
):
    rows, cols = one_gate.shape
    piece = norm_train.shape[1]
    part = cols // parts
    me, col = lax.axis_index("shard"), lax.axis_index("model")
    at = position_of(me, n)

    ones, others = (one_gate, one_up), (other_gate, other_up)
    finals, columns = (final_gate, final_up), (column_gate, column_up)

    loads = {}
    for w in range(2):
        for c in range(parts):
            span = pl.ds(c * part, part)
            pair = (
                pltpu.make_async_copy(ones[w].at[:, span], held_one.at[w, :, span], load_sem.at[w, c, 0]),
                pltpu.make_async_copy(others[w].at[:, span], held_other.at[w, :, span], load_sem.at[w, c, 1]),
            )
            for copy in pair:
                copy.start()
            loads[w, c] = pair

    barrier = pltpu.get_barrier_semaphore()
    for d in range(1, n):
        pl.semaphore_signal(barrier, inc=1, device_id=((me + d) % n, col), device_id_type=MESH)
    for d in range(1, k):
        pl.semaphore_signal(barrier, inc=1, device_id=(me, (col + d) % k), device_id_type=MESH)

    share[...] = jnp.broadcast_to(mix[...], (LANES, rows)).T

    maxima[1, parts - 1, 0, :, part:part + piece] = norm_train[...] + norm_step[...]

    def mixed(w, c):
        for copy in loads[w, c]:
            copy.wait()
        span = pl.ds(c * part, part)

        def step(g, top):
            lines = pl.ds(pl.multiple_of(g * 8, 8), 8)
            m = share[lines, 0:1]
            result = m * held_one[w, lines, span] + (1.0 - m) * held_other[w, lines, span]
            held_one[w, lines, span] = result
            return jnp.maximum(top, jnp.abs(result))

        top = lax.fori_loop(0, rows // 8, step, jnp.zeros((8, part), jnp.float32), unroll=4)
        maxima[w, c, 0, :, 0:part] = jnp.max(top, axis=0, keepdims=True)

    def tell(w, c):
        width = part + LANES if (w, c) == (1, parts - 1) else part
        copies = []
        for d in range(1, n):
            copy = pltpu.make_async_remote_copy(
                src_ref=maxima.at[w, c, 0, :, pl.ds(0, width)], dst_ref=maxima.at[w, c, d, :, pl.ds(0, width)],
                send_sem=max_send.at[w, c, d], recv_sem=max_recv.at[w, c, d],
                device_id=((me + d) % n, col), device_id_type=MESH,
            )
            copy.start()
            copies.append(copy)
        return copies

    def ring(way, hop, w, c):
        origin = index_at((at + (n - hop if way == 0 else hop)) % n, n)
        lines, span = pl.ds(pl.multiple_of(origin * rows, rows), rows), pl.ds(c * part, part)
        to = index_at((at + (1 if way == 0 else n - 1)) % n, n)
        return pltpu.make_async_remote_copy(
            src_ref=finals[w].at[lines, span], dst_ref=finals[w].at[lines, span],
            send_sem=ring_send.at[way, hop, w, c], recv_sem=ring_recv.at[way, hop, w, c],
            device_id=(to, col), device_id_type=MESH,
        )

    def scaled(w, c, inverse):
        span = pl.ds(c * part, part)

        def step(g, _):
            start = pl.multiple_of(g * 16, 16)
            to = pl.multiple_of(me * rows + g * 16, 16)
            finals[w][pl.ds(to, 16), span] = (held_one[w, pl.ds(start, 16), span] * inverse).astype(jnp.bfloat16)
            return 0

        lax.fori_loop(0, rows // 16, step, 0, unroll=2)

    units = [(w, c) for w in range(2) for c in range(parts)]
    told = {}
    for w, c in units:
        mixed(w, c)
        if (w, c) == units[0]:
            pl.semaphore_wait(barrier, n - 1 + k - 1)
        told[w, c] = tell(w, c)

    sent, norms = {}, []
    for w, c in units:
        for copy in told[w, c]:
            copy.wait_recv()
        column = jnp.max(maxima[w, c, :, :, 0:part], axis=0)
        columns[w][:, pl.ds(c * part, part)] = column
        scaled(w, c, 1.0 / column)
        for way in range(2):
            sent[way, 0, w, c] = ring(way, 0, w, c)
            sent[way, 0, w, c].start()

    for d in range(n):
        gains[0, pl.ds((me + (n - d)) % n, 1), :] = maxima[1, parts - 1, d, :, part:part + LANES]
    for d in range(1, k):
        copy = pltpu.make_async_remote_copy(
            src_ref=gains.at[0], dst_ref=gains.at[d],
            send_sem=norm_send.at[d], recv_sem=norm_recv.at[d],
            device_id=(me, (col + d) % k), device_id_type=MESH,
        )
        copy.start()
        norms.append(copy)
    for copy in norms:
        copy.wait_recv()
    gain = jnp.concatenate([gains[(col + (k - j)) % k][:, 0:piece] for j in range(k)], axis=1)
    if serve_norm.shape[1] == gain.shape[1]:
        serve_norm[...] = gain.astype(jnp.bfloat16)
    else:
        each = k * piece // LANES
        for i in range(n * each):
            at_lane = i % each * LANES
            gain_rows[i:i + 1, :] = gain[i // each:i // each + 1, at_lane:at_lane + LANES]
        serve_norm[...] = gain_rows[...].astype(jnp.bfloat16)

    for hop in range(1, n // 2 + 1):
        for w in range(2):
            for c in range(parts):
                for way in range(2):
                    if (way, hop - 1, w, c) not in sent:
                        continue
                    sent[way, hop - 1, w, c].wait_recv()
                    if hop < n // 2 - 1 or (hop == n // 2 - 1 and way == w):
                        sent[way, hop, w, c] = ring(way, hop, w, c)
                        sent[way, hop, w, c].start()

    for copy in sent.values():
        copy.wait_send()
    for copy in sum(told.values(), norms):
        copy.wait_send()


class Ring:
    def __init__(self, n, rows, blocks, sends, recvs):
        self.n, self.rows, self.blocks, self.sends, self.recvs = n, rows, blocks, sends, recvs
        self.me, self.col = lax.axis_index("shard"), lax.axis_index("model")
        self.at = position_of(self.me, n)

    def toward(self, way):
        return index_at((self.at + (1 if way == 0 else self.n - 1)) % self.n, self.n)

    def origin_of(self, way, hop):
        return index_at((self.at + (self.n - hop if way == 0 else hop)) % self.n, self.n)

    def place(self, b, origin, first, width):
        ref, start = self.blocks[b][0:2]
        lines = pl.ds(pl.multiple_of(origin * self.rows, self.rows), self.rows)
        return ref.at[lines, pl.ds(start + first, width)]

    def send(self, way, hop, b, first, width, source=None):
        part = self.place(b, self.origin_of(way, hop), first, width)
        pltpu.make_async_remote_copy(
            src_ref=part if source is None else source, dst_ref=part,
            send_sem=self.sends.at[way, b], recv_sem=self.recvs.at[hop, way, b],
            device_id=(self.toward(way), self.col), device_id_type=MESH,
        ).start()

    def arrived(self, way, hop, b, first, width):
        wait_for(self.place(b, self.origin_of(way, hop + 1), first, width), self.recvs.at[hop, way, b])

    def final_part(self, way, b):
        width = self.blocks[b][2]
        if b < 2:
            return (0, width) if way == b else None
        return (way * (width // 2), width // 2)

    def each(self, act):
        for i in range(len(self.blocks)):
            for way in range(2):
                b = (i, 1 - i if i < 2 else i)[way]
                only = self.blocks[b][4]
                if only is None:
                    act(way, b)
                else:
                    pl.when(only)(functools.partial(act, way, b))

    def go(self):
        last = self.n // 2 - 1
        for hop in range(1, last + 1):
            def forward(way, b, hop=hop):
                width = self.blocks[b][3 if hop == 1 else 2]
                part = (0, self.blocks[b][2]) if hop < last else self.final_part(way, b)
                if part is not None:
                    self.arrived(way, hop - 1, b, 0, width)
                    wait_for(self.place(b, self.me, 0, width), self.sends.at[way, b])
                    self.send(way, hop, b, *part)
            self.each(forward)

        def rest(way, b):
            if self.final_part(way, b) is None:
                self.arrived(way, last - 1, b, 0, self.blocks[b][2])

        def end(way, b):
            part = self.final_part(way, b)
            if part is not None:
                self.arrived(way, last, b, *part)

        def drain(way, b):
            part = self.final_part(way, b) or (0, self.blocks[b][2])
            wait_for(self.place(b, self.me, *part), self.sends.at[way, b])

        for act in (rest, end, drain):
            self.each(act)


def wait_for(ref, sem):
    pltpu.make_async_copy(ref, ref, sem).wait()


def near_kernel(
    n, k, units, direct, early,
    one_gate, other_gate, one_up, other_up, mix, norm_train, norm_step,
    final_gate, column_gate, column_up, serve_norm, own_up, extra,
    taken, result, mix_held, norm_held, share, raw, mine, heard, partial, whole, gains, gain_rows,
    load_sem, small_sem, raw_sem, max_send, max_recv, part_sem, whole_sem, norm_sem, ring_send, ring_recv,
):
    rows, cols = one_gate.shape
    piece = norm_train.shape[1]
    block = mine.shape[2]
    me, col = lax.axis_index("shard"), lax.axis_index("model")

    ones, others = (one_gate, one_up), (other_gate, other_up)
    columns = (column_gate, column_up)
    odd = leads(col)

    def peer(d):
        return ((me + d) % n, col)

    def load(u):
        w, first, width = units[u]
        span = pl.ds(first, width)
        for i, source in enumerate((ones[w], others[w])):
            pltpu.make_async_copy(source.at[:, span], taken.at[w, i, :, span], load_sem.at[u]).start()

    pltpu.make_async_copy(mix, mix_held, small_sem.at[0]).start()
    load(0)
    barrier = pltpu.get_barrier_semaphore()
    for d in range(1, n):
        pl.semaphore_signal(barrier, inc=1, device_id=peer(d), device_id_type=MESH)
    for d in range(1, k):
        pl.semaphore_signal(barrier, inc=1, device_id=(me, (col + d) % k), device_id_type=MESH)
    load(early)
    for u in range(1, early):
        load(u)
    for i, source in enumerate((norm_train, norm_step)):
        pltpu.make_async_copy(source, norm_held.at[i], small_sem.at[1]).start()

    wait_for(mix_held, small_sem.at[0])
    share[...] = jnp.broadcast_to(mix_held[...], (LANES, rows)).T

    def mixed(u):
        w, first, width = units[u]
        span = pl.ds(first, width)
        wait_for(taken.at[w, :, :, span], load_sem.at[u])

        def step(g, top):
            lines = pl.ds(pl.multiple_of(g * 8, 8), 8)
            m = share[lines, :]
            both = jnp.concatenate([m] * (width // LANES), axis=1)
            rest = jnp.concatenate([1.0 - m] * (width // LANES), axis=1)
            value = both * taken[w, 0, lines, span] + rest * taken[w, 1, lines, span]
            result[w, lines, span] = value
            return jnp.maximum(top, jnp.abs(value))

        top = lax.fori_loop(0, rows // 8, step, jnp.zeros((8, width), jnp.float32), unroll=4)
        top = jnp.max(top, axis=0, keepdims=True)
        done = 0
        while done < width:
            b, lane = (w * cols + first + done) // block, (first + done) % block
            take = min(block - lane, width - done)
            mine[b, :, lane:lane + take] = top[:, done:done + take]
            done += take

    def tell(u):
        for d in range(1, n):
            pltpu.make_async_remote_copy(
                src_ref=mine.at[u], dst_ref=heard.at[u, d],
                send_sem=max_send.at[0], recv_sem=max_recv.at[u], device_id=peer(d), device_id_type=MESH,
            ).start()

    def heard_of(u):
        wait_for(heard.at[u, pl.ds(1, n - 1)], max_recv.at[u])
        top = mine[u]
        for d in range(1, n):
            top = jnp.maximum(top, heard[u, d])
        return 1.0 / top

    e_weight, e_first, e_width = units[early]
    half = cols // 2
    shared = extra.shape[1]
    ring = Ring(
        n, rows,
        (
            (final_gate, 0, half, half, None), (final_gate, half, half, half - e_width, None),
            (extra, 0, shared, shared, odd),
        ),
        ring_send, ring_recv,
    )

    def scaled(target, origin, first, width, inverse, read):
        def step(g, _):
            start = pl.multiple_of(g * 16, 16)
            to = pl.multiple_of(origin * rows + g * 16, 16)
            target[pl.ds(to, 16), pl.ds(first, width)] = (read(pl.ds(start, 16)) * inverse).astype(jnp.bfloat16)
            return 0

        lax.fori_loop(0, rows // 16, step, 0, unroll=2)

    def held(w, first, width):
        return lambda lines: result[w, lines, pl.ds(first, width)]

    def begin(u, inverse):
        w, first, width = units[u]
        scaled(final_gate, me, first, width, inverse, held(w, first, width))
        for way in range(2):
            b = first // half
            ring.send(way, 0, b, first - b * half, width)

    mixed(0)
    pl.semaphore_wait(barrier, n - 1 + k - 1)
    tell(0)
    mixed(early)
    for way in range(2):
        pltpu.make_async_remote_copy(
            src_ref=result.at[e_weight, :, pl.ds(e_first, e_width)], dst_ref=raw.at[way],
            send_sem=raw_sem.at[0], recv_sem=raw_sem.at[1], device_id=(ring.toward(way), col), device_id_type=MESH,
        ).start()
    for u in range(1, direct):
        mixed(u)
        tell(u)
    for u in range(direct, early):
        mixed(u)
    for d in range(1, n):
        pltpu.make_async_remote_copy(
            src_ref=mine.at[(me + d) % n], dst_ref=partial.at[d],
            send_sem=part_sem.at[0], recv_sem=part_sem.at[1], device_id=peer(d), device_id_type=MESH,
        ).start()
    wait_for(norm_held, small_sem.at[1])

    begin(0, heard_of(0))

    wait_for(partial.at[pl.ds(1, n - 1)], part_sem.at[1])
    top = mine[me]
    for d in range(1, n):
        top = jnp.maximum(top, partial[d])
    whole[me, :, 0:block] = top
    whole[me, :, block:block + piece] = norm_held[0] + norm_held[1]
    for d in range(1, n):
        pltpu.make_async_remote_copy(
            src_ref=whole.at[me], dst_ref=whole.at[me],
            send_sem=whole_sem.at[0], recv_sem=whole_sem.at[1], device_id=peer(d), device_id_type=MESH,
        ).start()

    for u in range(1, direct):
        begin(u, heard_of(u))

    wait_for(whole.at[pl.ds(1, n - 1)], whole_sem.at[1])
    for b in range(n):
        w, first = b * block // cols, b * block % cols
        columns[w][:, first:first + block] = whole[b, :, 0:block]

    for u in range(direct, early):
        w, first, width = units[u]
        if w == 0:
            begin(u, 1.0 / columns[0][:, first:first + width])

    inverse_up = 1.0 / columns[1][...]
    scaled(own_up, 0, 0, cols, inverse_up, held(1, 0, cols))

    @pl.when(odd)
    def _():
        scaled(extra, me, 0, shared, inverse_up[:, 0:shared], held(1, 0, shared))
        for way in range(2):
            ring.send(way, 0, 2, 0, shared, own_up.at[:, pl.ds(0, shared)])

    inverse = 1.0 / columns[e_weight][:, e_first:e_first + e_width]
    wait_for(raw, raw_sem.at[1])
    for way in range(2):
        scaled(final_gate, ring.origin_of(way, 1), e_first, e_width, inverse, lambda lines: raw[way, lines, :])
    scaled(final_gate, me, e_first, e_width, inverse, held(e_weight, e_first, e_width))

    for d in range(n):
        gains[0, d:d + 1, :] = whole[d, :, block:block + LANES]
    for d in range(1, k):
        pltpu.make_async_remote_copy(
            src_ref=gains.at[0], dst_ref=gains.at[d], send_sem=norm_sem.at[0], recv_sem=norm_sem.at[1],
            device_id=(me, (col + d) % k), device_id_type=MESH,
        ).start()
    wait_for(gains.at[pl.ds(1, k - 1)], norm_sem.at[1])
    gain = jnp.concatenate([gains[(col + (k - j)) % k][:, 0:piece] for j in range(k)], axis=1)
    if serve_norm.shape[1] == gain.shape[1]:
        serve_norm[...] = gain.astype(jnp.bfloat16)
    else:
        each = k * piece // LANES
        for i in range(n * each):
            at_lane = i % each * LANES
            gain_rows[i:i + 1, :] = gain[i // each:i // each + 1, at_lane:at_lane + LANES]
        serve_norm[...] = gain_rows[...].astype(jnp.bfloat16)

    ring.go()
    wait_for(raw, raw_sem.at[0])
    wait_for(heard.at[:, pl.ds(1, n - 1)], max_send.at[0])
    wait_for(partial.at[pl.ds(1, n - 1)], part_sem.at[0])
    wait_for(whole.at[pl.ds(1, n - 1)], whole_sem.at[0])
    wait_for(gains.at[pl.ds(1, k - 1)], norm_sem.at[0])


def leads(col):
    return col % 2 == LEADER


def second_kernel(n, shared, own_up, after, final_up, ring_send, ring_recv):
    rows, cols = own_up.shape
    half = (cols - shared) // 2
    even = jnp.logical_not(leads(lax.axis_index("model")))
    ring = Ring(
        n, rows,
        (
            (final_up, shared, half, half, None), (final_up, shared + half, half, half, None),
            (final_up, 0, shared, shared, even),
        ),
        ring_send, ring_recv,
    )
    barrier = pltpu.get_barrier_semaphore()
    for way in range(2):
        pl.semaphore_signal(barrier, inc=1, device_id=(ring.toward(way), ring.col), device_id_type=MESH)
    pl.semaphore_wait(barrier, 2)

    def first_hop(way, b):
        _, start, width, _, _ = ring.blocks[b]
        ring.send(way, 0, b, 0, width, own_up.at[:, pl.ds(start, width)])

    ring.each(first_hop)

    def step(g, _):
        start = pl.multiple_of(g * 16, 16)
        final_up[pl.ds(pl.multiple_of(ring.me * rows + start, 16), 16), :] = own_up[pl.ds(start, 16), :]
        return 0

    lax.fori_loop(0, rows // 16, step, 0, unroll=2)
    ring.go()


def out(source, target, sem):
    pieces = PIECES if source.shape[0] > LANES else 1
    lines = source.shape[0] // pieces
    for p in range(pieces):
        span = pl.ds(p * lines, lines)
        pltpu.make_async_copy(source.at[span], target.at[span], sem).start()


def first_writer(final_gate, column_gate, column_up, serve_norm, extra, gate_out, gate_column, up_column, norm_out, up_out, after, sem):
    whole = ((final_gate, gate_out), (column_gate, gate_column), (column_up, up_column), (serve_norm, norm_out))
    lead = leads(lax.axis_index("model"))
    part = up_out.at[:, pl.ds(0, extra.shape[1])]
    for i, (source, target) in enumerate(whole):
        out(source, target, sem.at[i])
    pl.when(lead)(lambda: out(extra, part, sem.at[len(whole)]))
    after[...] = jnp.zeros_like(after)
    for i, (source, target) in enumerate(whole):
        pltpu.make_async_copy(source, target, sem.at[i]).wait()
    pl.when(lead)(lambda: pltpu.make_async_copy(extra, part, sem.at[len(whole)]).wait())


def last_writer(shared, final_up, up_in, up_out, sem):
    lead = leads(lax.axis_index("model"))
    cols = final_up.shape[1]

    def write(first):
        span = pl.ds(first, cols - first)
        out(final_up.at[:, span], up_out.at[:, span], sem.at[0])
        pltpu.make_async_copy(final_up.at[:, span], up_out.at[:, span], sem.at[0]).wait()

    pl.when(lead)(functools.partial(write, shared))
    pl.when(jnp.logical_not(lead))(functools.partial(write, 0))


def solution(mesh):
    n, k = mesh.shape["shard"], mesh.shape["model"]

    def local(one_gate, other_gate, one_up, other_up, mix_share, norm_train, norm_step):
        rows, cols = one_gate.shape
        piece = norm_train.shape[0]
        parts = 2 if n <= 8 else 1
        near = 4 < n <= 8
        norm_shape = (n * k * piece // LANES, LANES) if k * piece % LANES == 0 else (n, k * piece)
        shapes = [
            ((n * rows, cols), jnp.bfloat16), ((n * rows, cols), jnp.bfloat16),
            ((1, cols), jnp.float32), ((1, cols), jnp.float32), (norm_shape, jnp.bfloat16),
        ]
        hbm, vmem = pl.BlockSpec(memory_space=pltpu.HBM), pl.BlockSpec(memory_space=pltpu.VMEM)
        sems = pltpu.SemaphoreType.DMA
        gain_shapes = [
            pltpu.VMEM((k, n, LANES), jnp.float32),
            pltpu.VMEM((max(n * k * piece // LANES, 8), LANES), jnp.float32),
        ]
        operands = (
            one_gate, other_gate, one_up, other_up,
            mix_share.reshape(1, rows), norm_train.reshape(1, piece), norm_step.reshape(1, piece),
        )

        if near:
            block = 2 * cols // n
            e = cols // 16
            shared = cols // 8 * SHARED
            units = (
                (0, 0, block), (0, block, block), (0, 8 * e, 7 * e),
                (1, 0, 8 * e), (1, 8 * e, 8 * e), (0, 15 * e, e),
            )
            direct, early = 2, len(units) - 1
            final_gate, column_gate, column_up, serve_norm, own_up, extra = pl.pallas_call(
                functools.partial(near_kernel, n, k, units, direct, early),
                out_shape=[pltpu.VMEM(*shape) for shape in shapes[0:1] + shapes[2:5]] + [
                    pltpu.VMEM((rows, cols), jnp.bfloat16), pltpu.VMEM((n * rows, shared), jnp.bfloat16),
                ],
                in_specs=[hbm] * 7,
                out_specs=[vmem] * 6,
                scratch_shapes=[
                    pltpu.VMEM((2, 2, rows, cols), jnp.float32),
                    pltpu.VMEM((2, rows, cols), jnp.float32),
                    pltpu.VMEM((1, rows), jnp.float32), pltpu.VMEM((2, 1, piece), jnp.float32),
                    pltpu.VMEM((rows, LANES), jnp.float32),
                    pltpu.VMEM((2, rows, e), jnp.float32),
                    pltpu.VMEM((n, 1, block), jnp.float32),
                    pltpu.VMEM((direct, n, 1, block), jnp.float32),
                    pltpu.VMEM((n, 1, block), jnp.float32),
                    pltpu.VMEM((n, 1, block + LANES), jnp.float32),
                ] + gain_shapes + [
                    sems((len(units),)), sems((2,)), sems((2,)), sems((1,)), sems((direct,)), sems((2,)), sems((2,)), sems((2,)),
                    sems((2, 3)), sems((n // 2, 2, 3)),
                ],
                compiler_params=pltpu.CompilerParams(collective_id=0, has_side_effects=True, vmem_limit_bytes=(54 - SHARED) * 2**20),
            )(*operands)
            full = [jax.ShapeDtypeStruct(*shape) for shape in shapes]
            final_gate, column_gate, column_up, serve_norm, final_up, after = pl.pallas_call(
                first_writer,
                out_shape=[full[0], full[2], full[3], full[4], full[1], pltpu.VMEM((8, LANES), jnp.float32)],
                in_specs=[vmem] * 5,
                out_specs=[hbm] * 5 + [vmem],
                scratch_shapes=[sems((5,))],
                compiler_params=pltpu.CompilerParams(vmem_limit_bytes=2**20),
            )(final_gate, column_gate, column_up, serve_norm, extra)
            gathered = pl.pallas_call(
                functools.partial(second_kernel, n, shared),
                out_shape=pltpu.VMEM(*shapes[1]),
                in_specs=[vmem] * 2,
                out_specs=vmem,
                scratch_shapes=[sems((2, 3)), sems((n // 2, 2, 3))],
                compiler_params=pltpu.CompilerParams(collective_id=1, has_side_effects=True, vmem_limit_bytes=2**20),
            )(own_up, after)
            final_up = pl.pallas_call(
                functools.partial(last_writer, shared),
                out_shape=full[1],
                in_specs=[vmem, hbm],
                out_specs=hbm,
                scratch_shapes=[sems((1,))],
                input_output_aliases={1: 0},
                compiler_params=pltpu.CompilerParams(vmem_limit_bytes=2**20),
            )(gathered, final_up)
        else:
            final_gate, final_up, column_gate, column_up, serve_norm = pl.pallas_call(
                functools.partial(kernel, n, k, parts),
                out_shape=[jax.ShapeDtypeStruct(*shape) for shape in shapes],
                in_specs=[hbm] * 4 + [vmem] * 3,
                out_specs=[vmem] * 5,
                scratch_shapes=[pltpu.VMEM((2, rows, cols), jnp.float32)] * 2 + [
                    pltpu.VMEM((rows, LANES), jnp.float32),
                    pltpu.VMEM((2, parts, n, 1, cols // parts + LANES), jnp.float32),
                ] + gain_shapes + [
                    sems((2, parts, 2)), sems((2, parts, n)), sems((2, parts, n)), sems((k,)), sems((k,)),
                    sems((2, n // 2, 2, parts)), sems((2, n // 2, 2, parts)),
                ],
                compiler_params=pltpu.CompilerParams(collective_id=0, has_side_effects=True, vmem_limit_bytes=46 * 2**20),
            )(*operands)
        return (
            final_gate, final_up, column_gate.reshape(cols), column_up.reshape(cols),
            serve_norm.reshape(n * k * piece),
        )

    return jax.shard_map(
        local,
        mesh=mesh,
        in_specs=(
            P("shard", "model"), P("shard", "model"), P("shard", "model"), P("shard", "model"),
            P("shard"), P(("shard", "model")), P(("shard", "model")),
        ),
        out_specs=(P(None, "model"), P(None, "model"), P("model"), P("model"), P()),
        check_vma=False,
    )
```

```python
import functools

import jax
import jax.numpy as jnp
from jax import lax
from jax.experimental import pallas as pl
from jax.experimental.pallas import tpu as pltpu
from jax.sharding import PartitionSpec as P

MESH = pl.DeviceIdType.MESH
LANES = 128
SHARED = 3
MORE = 2
LEADER = 0
PIECES = 8


def position_of(index, n):
    return jnp.where(index % 2 == 0, index // 2, n - 1 - index // 2)


def index_at(position, n):
    return jnp.where(position < n // 2, 2 * position, 2 * (n - 1 - position) + 1)


def kernel(
    n, k, parts,
    one_gate, other_gate, one_up, other_up, mix, norm_train, norm_step,
    final_gate, final_up, column_gate, column_up, serve_norm,
    held_one, held_other, share, maxima, gains, gain_rows,
    load_sem, max_send, max_recv, norm_send, norm_recv, ring_send, ring_recv,
):
    rows, cols = one_gate.shape
    piece = norm_train.shape[1]
    part = cols // parts
    me, col = lax.axis_index("shard"), lax.axis_index("model")
    at = position_of(me, n)

    ones, others = (one_gate, one_up), (other_gate, other_up)
    finals, columns = (final_gate, final_up), (column_gate, column_up)

    loads = {}
    for w in range(2):
        for c in range(parts):
            span = pl.ds(c * part, part)
            pair = (
                pltpu.make_async_copy(ones[w].at[:, span], held_one.at[w, :, span], load_sem.at[w, c, 0]),
                pltpu.make_async_copy(others[w].at[:, span], held_other.at[w, :, span], load_sem.at[w, c, 1]),
            )
            for copy in pair:
                copy.start()
            loads[w, c] = pair

    barrier = pltpu.get_barrier_semaphore()
    for d in range(1, n):
        pl.semaphore_signal(barrier, inc=1, device_id=((me + d) % n, col), device_id_type=MESH)
    for d in range(1, k):
        pl.semaphore_signal(barrier, inc=1, device_id=(me, (col + d) % k), device_id_type=MESH)

    share[...] = jnp.broadcast_to(mix[...], (LANES, rows)).T

    maxima[1, parts - 1, 0, :, part:part + piece] = norm_train[...] + norm_step[...]

    def mixed(w, c):
        for copy in loads[w, c]:
            copy.wait()
        span = pl.ds(c * part, part)

        def step(g, top):
            lines = pl.ds(pl.multiple_of(g * 8, 8), 8)
            m = share[lines, 0:1]
            result = m * held_one[w, lines, span] + (1.0 - m) * held_other[w, lines, span]
            held_one[w, lines, span] = result
            return jnp.maximum(top, jnp.abs(result))

        top = lax.fori_loop(0, rows // 8, step, jnp.zeros((8, part), jnp.float32), unroll=4)
        maxima[w, c, 0, :, 0:part] = jnp.max(top, axis=0, keepdims=True)

    def tell(w, c):
        width = part + LANES if (w, c) == (1, parts - 1) else part
        copies = []
        for d in range(1, n):
            copy = pltpu.make_async_remote_copy(
                src_ref=maxima.at[w, c, 0, :, pl.ds(0, width)], dst_ref=maxima.at[w, c, d, :, pl.ds(0, width)],
                send_sem=max_send.at[w, c, d], recv_sem=max_recv.at[w, c, d],
                device_id=((me + d) % n, col), device_id_type=MESH,
            )
            copy.start()
            copies.append(copy)
        return copies

    def ring(way, hop, w, c):
        origin = index_at((at + (n - hop if way == 0 else hop)) % n, n)
        lines, span = pl.ds(pl.multiple_of(origin * rows, rows), rows), pl.ds(c * part, part)
        to = index_at((at + (1 if way == 0 else n - 1)) % n, n)
        return pltpu.make_async_remote_copy(
            src_ref=finals[w].at[lines, span], dst_ref=finals[w].at[lines, span],
            send_sem=ring_send.at[way, hop, w, c], recv_sem=ring_recv.at[way, hop, w, c],
            device_id=(to, col), device_id_type=MESH,
        )

    def scaled(w, c, inverse):
        span = pl.ds(c * part, part)

        def step(g, _):
            start = pl.multiple_of(g * 16, 16)
            to = pl.multiple_of(me * rows + g * 16, 16)
            finals[w][pl.ds(to, 16), span] = (held_one[w, pl.ds(start, 16), span] * inverse).astype(jnp.bfloat16)
            return 0

        lax.fori_loop(0, rows // 16, step, 0, unroll=2)

    units = [(w, c) for w in range(2) for c in range(parts)]
    told = {}
    for w, c in units:
        mixed(w, c)
        if (w, c) == units[0]:
            pl.semaphore_wait(barrier, n - 1 + k - 1)
        told[w, c] = tell(w, c)

    sent, norms = {}, []
    for w, c in units:
        for copy in told[w, c]:
            copy.wait_recv()
        column = jnp.max(maxima[w, c, :, :, 0:part], axis=0)
        columns[w][:, pl.ds(c * part, part)] = column
        scaled(w, c, 1.0 / column)
        for way in range(2):
            sent[way, 0, w, c] = ring(way, 0, w, c)
            sent[way, 0, w, c].start()

    for d in range(n):
        gains[0, pl.ds((me + (n - d)) % n, 1), :] = maxima[1, parts - 1, d, :, part:part + LANES]
    for d in range(1, k):
        copy = pltpu.make_async_remote_copy(
            src_ref=gains.at[0], dst_ref=gains.at[d],
            send_sem=norm_send.at[d], recv_sem=norm_recv.at[d],
            device_id=(me, (col + d) % k), device_id_type=MESH,
        )
        copy.start()
        norms.append(copy)
    for copy in norms:
        copy.wait_recv()
    gain = jnp.concatenate([gains[(col + (k - j)) % k][:, 0:piece] for j in range(k)], axis=1)
    if serve_norm.shape[1] == gain.shape[1]:
        serve_norm[...] = gain.astype(jnp.bfloat16)
    else:
        each = k * piece // LANES
        for i in range(n * each):
            at_lane = i % each * LANES
            gain_rows[i:i + 1, :] = gain[i // each:i // each + 1, at_lane:at_lane + LANES]
        serve_norm[...] = gain_rows[...].astype(jnp.bfloat16)

    for hop in range(1, n // 2 + 1):
        for w in range(2):
            for c in range(parts):
                for way in range(2):
                    if (way, hop - 1, w, c) not in sent:
                        continue
                    sent[way, hop - 1, w, c].wait_recv()
                    if hop < n // 2 - 1 or (hop == n // 2 - 1 and way == w):
                        sent[way, hop, w, c] = ring(way, hop, w, c)
                        sent[way, hop, w, c].start()

    for copy in sent.values():
        copy.wait_send()
    for copy in sum(told.values(), norms):
        copy.wait_send()


class Ring:
    def __init__(self, n, rows, blocks, sends, recvs):
        self.n, self.rows, self.blocks, self.sends, self.recvs = n, rows, blocks, sends, recvs
        self.me, self.col = lax.axis_index("shard"), lax.axis_index("model")
        self.at = position_of(self.me, n)

    def toward(self, way):
        return index_at((self.at + (1 if way == 0 else self.n - 1)) % self.n, self.n)

    def origin_of(self, way, hop):
        return index_at((self.at + (self.n - hop if way == 0 else hop)) % self.n, self.n)

    def place(self, b, origin, first, width):
        ref, start = self.blocks[b][0:2]
        lines = pl.ds(pl.multiple_of(origin * self.rows, self.rows), self.rows)
        return ref.at[lines, pl.ds(start + first, width)]

    def send(self, way, hop, b, first, width, source=None):
        part = self.place(b, self.origin_of(way, hop), first, width)
        pltpu.make_async_remote_copy(
            src_ref=part if source is None else source, dst_ref=part,
            send_sem=self.sends.at[way, b], recv_sem=self.recvs.at[hop, way, b],
            device_id=(self.toward(way), self.col), device_id_type=MESH,
        ).start()

    def arrived(self, way, hop, b, first, width):
        wait_for(self.place(b, self.origin_of(way, hop + 1), first, width), self.recvs.at[hop, way, b])

    def final_part(self, way, b):
        width = self.blocks[b][2]
        if b < 2:
            return (0, width) if way == b else None
        return (way * (width // 2), width // 2)

    def each(self, act):
        for i in range(len(self.blocks)):
            for way in range(2):
                b = (i, 1 - i if i < 2 else i)[way]
                only = self.blocks[b][4]
                if only is None:
                    act(way, b)
                else:
                    pl.when(only)(functools.partial(act, way, b))

    def go(self):
        last = self.n // 2 - 1
        for hop in range(1, last + 1):
            def forward(way, b, hop=hop):
                width = self.blocks[b][3 if hop == 1 else 2]
                part = (0, self.blocks[b][2]) if hop < last else self.final_part(way, b)
                if part is not None:
                    self.arrived(way, hop - 1, b, 0, width)
                    wait_for(self.place(b, self.me, 0, width), self.sends.at[way, b])
                    self.send(way, hop, b, *part)
            self.each(forward)

        def rest(way, b):
            if self.final_part(way, b) is None:
                self.arrived(way, last - 1, b, 0, self.blocks[b][2])

        def end(way, b):
            part = self.final_part(way, b)
            if part is not None:
                self.arrived(way, last, b, *part)

        def drain(way, b):
            part = self.final_part(way, b) or (0, self.blocks[b][2])
            wait_for(self.place(b, self.me, *part), self.sends.at[way, b])

        for act in (rest, end, drain):
            self.each(act)


def wait_for(ref, sem):
    pltpu.make_async_copy(ref, ref, sem).wait()


def near_kernel(
    n, k, units, direct, early, shared,
    one_gate, other_gate, one_up, other_up, mix, norm_train, norm_step,
    final_gate, column_gate, column_up, serve_norm, own_up, extra,
    taken, result, mix_held, norm_held, share, raw, mine, heard, partial, whole, gains, gain_rows,
    load_sem, small_sem, raw_sem, max_send, max_recv, part_sem, whole_sem, norm_sem, ring_send, ring_recv,
):
    rows, cols = one_gate.shape
    piece = norm_train.shape[1]
    block = mine.shape[2]
    me, col = lax.axis_index("shard"), lax.axis_index("model")

    ones, others = (one_gate, one_up), (other_gate, other_up)
    columns = (column_gate, column_up)
    lead = leads(col)

    def peer(d):
        return ((me + d) % n, col)

    def load(u):
        w, first, width = units[u]
        span = pl.ds(first, width)
        for i, source in enumerate((ones[w], others[w])):
            pltpu.make_async_copy(source.at[:, span], taken.at[w, i, :, span], load_sem.at[u]).start()

    pltpu.make_async_copy(mix, mix_held, small_sem.at[0]).start()
    load(0)
    barrier = pltpu.get_barrier_semaphore()
    for d in range(1, n):
        pl.semaphore_signal(barrier, inc=1, device_id=peer(d), device_id_type=MESH)
    for d in range(1, k):
        pl.semaphore_signal(barrier, inc=1, device_id=(me, (col + d) % k), device_id_type=MESH)
    load(early)
    for u in range(1, early):
        load(u)
    for i, source in enumerate((norm_train, norm_step)):
        pltpu.make_async_copy(source, norm_held.at[i], small_sem.at[1]).start()

    wait_for(mix_held, small_sem.at[0])
    share[...] = jnp.broadcast_to(mix_held[...], (LANES, rows)).T

    def mixed(u):
        w, first, width = units[u]
        span = pl.ds(first, width)
        wait_for(taken.at[w, :, :, span], load_sem.at[u])

        def step(g, top):
            lines = pl.ds(pl.multiple_of(g * 8, 8), 8)
            m = share[lines, :]
            both = jnp.concatenate([m] * (width // LANES), axis=1)
            rest = jnp.concatenate([1.0 - m] * (width // LANES), axis=1)
            value = both * taken[w, 0, lines, span] + rest * taken[w, 1, lines, span]
            result[w, lines, span] = value
            return jnp.maximum(top, jnp.abs(value))

        top = lax.fori_loop(0, rows // 8, step, jnp.zeros((8, width), jnp.float32), unroll=4)
        top = jnp.max(top, axis=0, keepdims=True)
        done = 0
        while done < width:
            b, lane = (w * cols + first + done) // block, (first + done) % block
            take = min(block - lane, width - done)
            mine[b, :, lane:lane + take] = top[:, done:done + take]
            done += take

    def tell(u):
        for d in range(1, n):
            pltpu.make_async_remote_copy(
                src_ref=mine.at[u], dst_ref=heard.at[u, d],
                send_sem=max_send.at[0], recv_sem=max_recv.at[u], device_id=peer(d), device_id_type=MESH,
            ).start()

    def heard_of(u):
        wait_for(heard.at[u, pl.ds(1, n - 1)], max_recv.at[u])
        top = mine[u]
        for d in range(1, n):
            top = jnp.maximum(top, heard[u, d])
        return 1.0 / top

    e_weight, e_first, e_width = units[early]
    half = cols // 2
    total = extra.shape[1]
    ring = Ring(
        n, rows,
        (
            (final_gate, 0, half, half, None), (final_gate, half, half, half - e_width, None),
            (extra, 0, shared, shared, None), (extra, shared, total - shared, total - shared, lead),
        ),
        ring_send, ring_recv,
    )

    def scaled(target, origin, first, width, inverse, read):
        def step(g, _):
            start = pl.multiple_of(g * 16, 16)
            to = pl.multiple_of(origin * rows + g * 16, 16)
            target[pl.ds(to, 16), pl.ds(first, width)] = (read(pl.ds(start, 16)) * inverse).astype(jnp.bfloat16)
            return 0

        lax.fori_loop(0, rows // 16, step, 0, unroll=2)

    def held(w, first, width):
        return lambda lines: result[w, lines, pl.ds(first, width)]

    def begin(u, inverse):
        w, first, width = units[u]
        scaled(final_gate, me, first, width, inverse, held(w, first, width))
        for way in range(2):
            b = first // half
            ring.send(way, 0, b, first - b * half, width)

    mixed(0)
    pl.semaphore_wait(barrier, n - 1 + k - 1)
    tell(0)
    mixed(early)
    for way in range(2):
        pltpu.make_async_remote_copy(
            src_ref=result.at[e_weight, :, pl.ds(e_first, e_width)], dst_ref=raw.at[way],
            send_sem=raw_sem.at[0], recv_sem=raw_sem.at[1], device_id=(ring.toward(way), col), device_id_type=MESH,
        ).start()
    for u in range(1, direct):
        mixed(u)
        tell(u)
    for u in range(direct, early):
        mixed(u)
    for d in range(1, n):
        pltpu.make_async_remote_copy(
            src_ref=mine.at[(me + d) % n], dst_ref=partial.at[d],
            send_sem=part_sem.at[0], recv_sem=part_sem.at[1], device_id=peer(d), device_id_type=MESH,
        ).start()
    wait_for(norm_held, small_sem.at[1])

    begin(0, heard_of(0))

    wait_for(partial.at[pl.ds(1, n - 1)], part_sem.at[1])
    top = mine[me]
    for d in range(1, n):
        top = jnp.maximum(top, partial[d])
    whole[me, :, 0:block] = top
    whole[me, :, block:block + piece] = norm_held[0] + norm_held[1]
    for d in range(1, n):
        pltpu.make_async_remote_copy(
            src_ref=whole.at[me], dst_ref=whole.at[me],
            send_sem=whole_sem.at[0], recv_sem=whole_sem.at[1], device_id=peer(d), device_id_type=MESH,
        ).start()

    for u in range(1, direct):
        begin(u, heard_of(u))

    wait_for(whole.at[pl.ds(1, n - 1)], whole_sem.at[1])
    for b in range(n):
        w, first = b * block // cols, b * block % cols
        columns[w][:, first:first + block] = whole[b, :, 0:block]

    for u in range(direct, early):
        w, first, width = units[u]
        if w == 0:
            begin(u, 1.0 / columns[0][:, first:first + width])

    inverse_up = 1.0 / columns[1][...]
    scaled(own_up, 0, 0, cols, inverse_up, held(1, 0, cols))

    def begin_up(b):
        _, first, width = ring.blocks[b][0:3]
        scaled(extra, me, first, width, inverse_up[:, first:first + width], held(1, first, width))
        for way in range(2):
            ring.send(way, 0, b, 0, width, own_up.at[:, pl.ds(first, width)])

    begin_up(2)
    pl.when(lead)(lambda: begin_up(3))

    inverse = 1.0 / columns[e_weight][:, e_first:e_first + e_width]
    wait_for(raw, raw_sem.at[1])
    for way in range(2):
        scaled(final_gate, ring.origin_of(way, 1), e_first, e_width, inverse, lambda lines: raw[way, lines, :])
    scaled(final_gate, me, e_first, e_width, inverse, held(e_weight, e_first, e_width))

    for d in range(n):
        gains[0, d:d + 1, :] = whole[d, :, block:block + LANES]
    for d in range(1, k):
        pltpu.make_async_remote_copy(
            src_ref=gains.at[0], dst_ref=gains.at[d], send_sem=norm_sem.at[0], recv_sem=norm_sem.at[1],
            device_id=(me, (col + d) % k), device_id_type=MESH,
        ).start()
    wait_for(gains.at[pl.ds(1, k - 1)], norm_sem.at[1])
    gain = jnp.concatenate([gains[(col + (k - j)) % k][:, 0:piece] for j in range(k)], axis=1)
    if serve_norm.shape[1] == gain.shape[1]:
        serve_norm[...] = gain.astype(jnp.bfloat16)
    else:
        each = k * piece // LANES
        for i in range(n * each):
            at_lane = i % each * LANES
            gain_rows[i:i + 1, :] = gain[i // each:i // each + 1, at_lane:at_lane + LANES]
        serve_norm[...] = gain_rows[...].astype(jnp.bfloat16)

    ring.go()
    wait_for(raw, raw_sem.at[0])
    wait_for(heard.at[:, pl.ds(1, n - 1)], max_send.at[0])
    wait_for(partial.at[pl.ds(1, n - 1)], part_sem.at[0])
    wait_for(whole.at[pl.ds(1, n - 1)], whole_sem.at[0])
    wait_for(gains.at[pl.ds(1, k - 1)], norm_sem.at[0])


def leads(col):
    return col % 2 == LEADER


def second_kernel(n, shared, total, own_up, after, final_up, ring_send, ring_recv):
    rows, cols = own_up.shape
    half = (cols - total) // 2
    even = jnp.logical_not(leads(lax.axis_index("model")))
    ring = Ring(
        n, rows,
        (
            (final_up, total, half, half, None), (final_up, total + half, half, half, None),
            (final_up, shared, total - shared, total - shared, even),
        ),
        ring_send, ring_recv,
    )
    barrier = pltpu.get_barrier_semaphore()
    for way in range(2):
        pl.semaphore_signal(barrier, inc=1, device_id=(ring.toward(way), ring.col), device_id_type=MESH)
    pl.semaphore_wait(barrier, 2)

    def first_hop(way, b):
        _, start, width, _, _ = ring.blocks[b]
        ring.send(way, 0, b, 0, width, own_up.at[:, pl.ds(start, width)])

    ring.each(first_hop)

    def step(g, _):
        start = pl.multiple_of(g * 16, 16)
        final_up[pl.ds(pl.multiple_of(ring.me * rows + start, 16), 16), :] = own_up[pl.ds(start, 16), :]
        return 0

    lax.fori_loop(0, rows // 16, step, 0, unroll=2)
    ring.go()


def out(source, target, sem):
    pieces = PIECES if source.shape[0] > LANES else 1
    lines = source.shape[0] // pieces
    for p in range(pieces):
        span = pl.ds(p * lines, lines)
        pltpu.make_async_copy(source.at[span], target.at[span], sem).start()


def by_role(act, shared, total):
    lead = leads(lax.axis_index("model"))
    pl.when(lead)(functools.partial(act, total))
    pl.when(jnp.logical_not(lead))(functools.partial(act, shared))


def first_writer(shared, final_gate, column_gate, column_up, serve_norm, extra, gate_out, gate_column, up_column, norm_out, up_out, after, sem):
    whole = ((final_gate, gate_out), (column_gate, gate_column), (column_up, up_column), (serve_norm, norm_out))
    for i, (source, target) in enumerate(whole):
        out(source, target, sem.at[i])
    after[...] = jnp.zeros_like(after)

    def write(width):
        source, target = extra.at[:, pl.ds(0, width)], up_out.at[:, pl.ds(0, width)]
        out(source, target, sem.at[len(whole)])
        pltpu.make_async_copy(source, target, sem.at[len(whole)]).wait()

    by_role(write, shared, extra.shape[1])
    for i, (source, target) in enumerate(whole):
        pltpu.make_async_copy(source, target, sem.at[i]).wait()


def last_writer(shared, total, final_up, up_in, up_out, sem):
    cols = final_up.shape[1]

    def write(first):
        span = pl.ds(first, cols - first)
        out(final_up.at[:, span], up_out.at[:, span], sem.at[0])
        pltpu.make_async_copy(final_up.at[:, span], up_out.at[:, span], sem.at[0]).wait()

    by_role(write, shared, total)


def solution(mesh):
    n, k = mesh.shape["shard"], mesh.shape["model"]

    def local(one_gate, other_gate, one_up, other_up, mix_share, norm_train, norm_step):
        rows, cols = one_gate.shape
        piece = norm_train.shape[0]
        parts = 2 if n <= 8 else 1
        near = 4 < n <= 8
        norm_shape = (n * k * piece // LANES, LANES) if k * piece % LANES == 0 else (n, k * piece)
        shapes = [
            ((n * rows, cols), jnp.bfloat16), ((n * rows, cols), jnp.bfloat16),
            ((1, cols), jnp.float32), ((1, cols), jnp.float32), (norm_shape, jnp.bfloat16),
        ]
        hbm, vmem = pl.BlockSpec(memory_space=pltpu.HBM), pl.BlockSpec(memory_space=pltpu.VMEM)
        sems = pltpu.SemaphoreType.DMA
        gain_shapes = [
            pltpu.VMEM((k, n, LANES), jnp.float32),
            pltpu.VMEM((max(n * k * piece // LANES, 8), LANES), jnp.float32),
        ]
        operands = (
            one_gate, other_gate, one_up, other_up,
            mix_share.reshape(1, rows), norm_train.reshape(1, piece), norm_step.reshape(1, piece),
        )

        if near:
            block = 2 * cols // n
            e = cols // 16
            shared, total = cols // 8 * SHARED, cols // 8 * (SHARED + MORE)
            units = (
                (0, 0, block), (0, block, block), (0, 8 * e, 7 * e),
                (1, 0, 8 * e), (1, 8 * e, 8 * e), (0, 15 * e, e),
            )
            direct, early = 2, len(units) - 1
            final_gate, column_gate, column_up, serve_norm, own_up, extra = pl.pallas_call(
                functools.partial(near_kernel, n, k, units, direct, early, shared),
                out_shape=[pltpu.VMEM(*shape) for shape in shapes[0:1] + shapes[2:5]] + [
                    pltpu.VMEM((rows, cols), jnp.bfloat16), pltpu.VMEM((n * rows, total), jnp.bfloat16),
                ],
                in_specs=[hbm] * 7,
                out_specs=[vmem] * 6,
                scratch_shapes=[
                    pltpu.VMEM((2, 2, rows, cols), jnp.float32),
                    pltpu.VMEM((2, rows, cols), jnp.float32),
                    pltpu.VMEM((1, rows), jnp.float32), pltpu.VMEM((2, 1, piece), jnp.float32),
                    pltpu.VMEM((rows, LANES), jnp.float32),
                    pltpu.VMEM((2, rows, e), jnp.float32),
                    pltpu.VMEM((n, 1, block), jnp.float32),
                    pltpu.VMEM((direct, n, 1, block), jnp.float32),
                    pltpu.VMEM((n, 1, block), jnp.float32),
                    pltpu.VMEM((n, 1, block + LANES), jnp.float32),
                ] + gain_shapes + [
                    sems((len(units),)), sems((2,)), sems((2,)), sems((1,)), sems((direct,)), sems((2,)), sems((2,)), sems((2,)),
                    sems((2, 4)), sems((n // 2, 2, 4)),
                ],
                compiler_params=pltpu.CompilerParams(
                    collective_id=0, has_side_effects=True, vmem_limit_bytes=(54 - SHARED - MORE) * 2**20
                ),
            )(*operands)
            full = [jax.ShapeDtypeStruct(*shape) for shape in shapes]
            final_gate, column_gate, column_up, serve_norm, final_up, after = pl.pallas_call(
                functools.partial(first_writer, shared),
                out_shape=[full[0], full[2], full[3], full[4], full[1], pltpu.VMEM((8, LANES), jnp.float32)],
                in_specs=[vmem] * 5,
                out_specs=[hbm] * 5 + [vmem],
                scratch_shapes=[sems((5,))],
                compiler_params=pltpu.CompilerParams(vmem_limit_bytes=2**20),
            )(final_gate, column_gate, column_up, serve_norm, extra)
            gathered = pl.pallas_call(
                functools.partial(second_kernel, n, shared, total),
                out_shape=pltpu.VMEM(*shapes[1]),
                in_specs=[vmem] * 2,
                out_specs=vmem,
                scratch_shapes=[sems((2, 3)), sems((n // 2, 2, 3))],
                compiler_params=pltpu.CompilerParams(collective_id=1, has_side_effects=True, vmem_limit_bytes=2**20),
            )(own_up, after)
            final_up = pl.pallas_call(
                functools.partial(last_writer, shared, total),
                out_shape=full[1],
                in_specs=[vmem, hbm],
                out_specs=hbm,
                scratch_shapes=[sems((1,))],
                input_output_aliases={1: 0},
                compiler_params=pltpu.CompilerParams(vmem_limit_bytes=2**20),
            )(gathered, final_up)
        else:
            final_gate, final_up, column_gate, column_up, serve_norm = pl.pallas_call(
                functools.partial(kernel, n, k, parts),
                out_shape=[jax.ShapeDtypeStruct(*shape) for shape in shapes],
                in_specs=[hbm] * 4 + [vmem] * 3,
                out_specs=[vmem] * 5,
                scratch_shapes=[pltpu.VMEM((2, rows, cols), jnp.float32)] * 2 + [
                    pltpu.VMEM((rows, LANES), jnp.float32),
                    pltpu.VMEM((2, parts, n, 1, cols // parts + LANES), jnp.float32),
                ] + gain_shapes + [
                    sems((2, parts, 2)), sems((2, parts, n)), sems((2, parts, n)), sems((k,)), sems((k,)),
                    sems((2, n // 2, 2, parts)), sems((2, n // 2, 2, parts)),
                ],
                compiler_params=pltpu.CompilerParams(collective_id=0, has_side_effects=True, vmem_limit_bytes=46 * 2**20),
            )(*operands)
        return (
            final_gate, final_up, column_gate.reshape(cols), column_up.reshape(cols),
            serve_norm.reshape(n * k * piece),
        )

    return jax.shard_map(
        local,
        mesh=mesh,
        in_specs=(
            P("shard", "model"), P("shard", "model"), P("shard", "model"), P("shard", "model"),
            P("shard"), P(("shard", "model")), P(("shard", "model")),
        ),
        out_specs=(P(None, "model"), P(None, "model"), P("model"), P("model"), P()),
        check_vma=False,
    )
```
